32 devices in a mesh: expert: 8 (over y, x, core), dp: 4 (over z).
Axes of the slice: x: 2, y: 2, z: 4, core: 2. Of those that a mesh axis runs over, the one named last changes fastest.
Arguments:
- out_grads: bfloat16 [4, 1024, 7168], P('dp', 'expert'), may hold values from -6 to 6
- expert_ids: int32 [4, 1024, 8], P('dp', 'expert'), may hold values from 0 to 63, all different within a row; in each aligned block of 128 rows (0 to 127, 128 to 255, ..., all dimensions but the last counted through in order) at most 24 rows name the same one
- gate_probs: float32 [4, 1024, 8], P('dp', 'expert'), may hold values from 0.05 to 0.5
- hidden_acts: bfloat16 [4, 64, 192, 2048], P('dp', 'expert'), may hold values from -6 to 6
- q_previous: bfloat16 [64, 32, 7168], P('expert'), may hold values from -0.0625 to 0.0625
Outputs:
- new_basis: float32 [64, 32, 2048], P('expert')
- q_update: float32 [64, 32, 7168], P('expert', None, 'dp')
The draws below stay inside these ranges and needn't reach their ends.
Inputs may be any that keep to these rules, and one draw needn't show every extreme that they name: `expert_ids`: each row names 8 different experts; among the rows of one device no expert is named more than 24 times.
All inputs are finite; a program needn't handle non-finite values.
Results may differ from the reference program's by a relative error of at most 0.014.
Values may be sent and summed in bfloat16 or wider, within the bound.
A program may use at most 192 MiB of HBM per device.

```python
import math
import jax
import jax.numpy as jnp
import numpy as np
from jax import lax

D = 7168
FF = 2048
TOP = 8
RANK = 32
TOK_DEV = 128
EXPERTS = 64
CAP = 24
SLOTS = 192
TOK_EXP = 1024
N_EXPERT = 8
N_DP = 4


def steps_of(key, extent, shards, smallest, top_value):
    factor_of, own = 1.0, jax.random.fold_in(key, 6)
    for dim, parts in shards:
        heights = jnp.exp(jax.random.uniform(jax.random.fold_in(own, dim), (parts,), jnp.float32, smallest / len(shards), top_value / len(shards)))
        factor_of = factor_of * jnp.repeat(heights, extent[dim] // parts).reshape([-1 if axis == dim else 1 for axis in range(len(extent))])
    return factor_of


def routed_block(rng, own, number, rows, count, top, limit, skew):
    ranking = jax.random.permutation(rng, count)
    crowded, usual = portions_of(count, rows * top, limit, skew, True), portions_of(count, rows * top, limit, skew, False)
    places = jnp.arange(count)

    def named(tallies, rotation):
        used = int((tallies > 0).sum())
        fixed = max(1, used // 4)
        passed = fixed + (places - fixed + rotation * (used - fixed)) % max(1, count - fixed)
        return jnp.zeros((count,), jnp.int32).at[ranking[jnp.where(places < fixed, places, passed)]].set(jnp.asarray(tallies, jnp.int32))

    tallies = jnp.where(number % 4 == 0, named(crowded, number // 4), named(usual, number - number // 4 - 1))
    mixed = jax.random.permutation(jax.random.fold_in(own, 3), count)
    source_of, sink = mixed[0:count // 2 * 2:2], mixed[1:count // 2 * 2:2]
    room = jnp.minimum(tallies[source_of] - 1, limit - tallies[sink]) // 2
    room = jnp.where((source_of == ranking[0]) | (sink == ranking[0]) | (tallies[sink] == 0), 0, jnp.maximum(room, 0))
    passed = jax.random.randint(jax.random.fold_in(own, 4), (count // 2,), 0, 1 << 20) % (room + 1)
    tallies = tallies.at[source_of].add(-passed).at[sink].add(passed)
    labels = jnp.searchsorted(jnp.cumsum(tallies), jnp.arange(rows * top), side="right").astype(jnp.int32)
    grid = labels.reshape(top, rows).T
    grid = grid[jax.random.permutation(jax.random.fold_in(own, 1), rows)]
    rotation = jax.random.randint(jax.random.fold_in(own, 2), (rows, 1), 0, top)
    return jnp.take_along_axis(grid, (jnp.arange(top)[None, :] + rotation) % top, axis=1)


def portions_of(number_of, total, bound, slope, full):
    weights = [(1 << 20) // math.isqrt(grade ** slope) + 1 for grade in range(1, number_of + 1)]
    largest = bound if full else min(bound, max(-(-total // number_of), total * weights[0] // sum(weights)))
    least = 1 if total - largest >= number_of - 1 else 0
    given, surplus = [largest] + [least] * (number_of - 1), total - largest - least * (number_of - 1)
    while surplus > 0:
        free = [i for i in range(1, number_of) if given[i] < largest] or [i for i in range(1, number_of) if given[i] < bound]
        mass, budget = sum([weights[i] for i in free]), surplus
        for i in free:
            more = min(bound - given[i], max(1, budget * weights[i] // mass), surplus)
            given[i] = given[i] + more
            surplus = surplus - more
    return np.array(given)


def noise(key, shape, deviation, bound, cuts=(), kind=jnp.bfloat16):
    factor_of = steps_of(key, shape, cuts, -0.22, 0.18) if cuts else 1.0
    result = jax.random.normal(key, shape, jnp.float32) * deviation * factor_of
    return jnp.minimum(jnp.maximum(result, -bound), bound).astype(kind)


def setup_inputs(seed: int = 0) -> dict:
    arg_keys = jax.random.split(jax.random.key(seed), 6)
    out_grads = noise(arg_keys[0], (N_DP, TOK_EXP, D), 1.0, 6.0, ((0, 4), (1, 8)))
    expert_ids_keys = jax.random.split(jax.random.fold_in(arg_keys[1], 1), N_DP * TOK_EXP // TOK_DEV)
    expert_ids_turns = jax.random.permutation(jax.random.fold_in(arg_keys[1], 3), N_DP * TOK_EXP // TOK_DEV)
    expert_ids = jax.vmap(lambda own, number: routed_block(jax.random.fold_in(arg_keys[1], 2), own, number, TOK_DEV, EXPERTS, TOP, CAP, 1))(expert_ids_keys, expert_ids_turns).reshape((N_DP, TOK_EXP, TOP))
    gate_probs = jnp.clip(0.05 + 0.45 * jax.random.uniform(arg_keys[2], (N_DP, TOK_EXP, TOP), jnp.float32) ** steps_of(arg_keys[2], (N_DP, TOK_EXP, TOP), ((0, 4), (1, 8)), -0.2, 0.2), 0.05, 0.5)
    hidden_acts = noise(arg_keys[3], (N_DP, EXPERTS, SLOTS, FF), 1.0, 6.0, ((0, 4), (1, 8)))
    q_previous = noise(arg_keys[4], (EXPERTS, RANK, D), D ** -0.5, 0.0625, ((0, 8),))
    return {"out_grads": out_grads, "expert_ids": expert_ids, "gate_probs": gate_probs, "hidden_acts": hidden_acts, "q_previous": q_previous}


def to_half(values):
    return lax.optimization_barrier(values.astype(jnp.bfloat16))

def slot_tables(route_ids, gate_values, num_experts, capacity):
    flat_ids = route_ids.reshape(-1)
    row_count = flat_ids.shape[0]
    top_k = route_ids.shape[-1]
    one_hot = (flat_ids[:, None] == jnp.arange(num_experts, dtype=jnp.int32)[None, :]).astype(jnp.int32)
    earlier = jnp.cumsum(one_hot, axis=0) - one_hot
    position = lax.optimization_barrier(jnp.sum(earlier * one_hot, axis=1)).astype(jnp.int32)
    slot_index = (flat_ids * capacity + position).astype(jnp.int32)
    token_of = jnp.zeros((num_experts * capacity,), jnp.int32).at[slot_index].set((jnp.arange(row_count, dtype=jnp.int32) // top_k).astype(jnp.int32))
    gate_of = jnp.zeros((num_experts * capacity,), jnp.float32).at[slot_index].set(gate_values.reshape(-1).astype(jnp.float32))
    return (token_of, gate_of)

def reference(out_grads, expert_ids, gate_probs, hidden_acts, q_previous):
    grads_blocks = out_grads.reshape(N_DP, N_EXPERT, TOK_DEV, D)
    id_blocks = expert_ids.reshape(N_DP, N_EXPERT, TOK_DEV, TOP)
    gate_blocks = gate_probs.reshape(N_DP, N_EXPERT, TOK_DEV, TOP)
    tables = jax.vmap(jax.vmap(lambda ids, gts: slot_tables(ids, gts, EXPERTS, CAP)))
    token_of, gate_of = tables(id_blocks, gate_blocks)

    def pick_rows(grads_one, tokens_one):
        return jnp.take(grads_one, tokens_one, axis=0)

    def one_expert(expert_num):
        start = (expert_num * CAP).astype(jnp.int32)
        tokens_here = lax.dynamic_slice_in_dim(token_of, start, CAP, 2)
        gates_here = lax.dynamic_slice_in_dim(gate_of, start, CAP, 2)
        picked = jax.vmap(jax.vmap(pick_rows))(grads_blocks, tokens_here)
        routed = to_half(picked.astype(jnp.float32) * gates_here[..., None]).reshape(N_DP, SLOTS, D)
        hidden_here = lax.dynamic_index_in_dim(hidden_acts, expert_num, 1, keepdims=False)
        q_here = lax.dynamic_index_in_dim(q_previous, expert_num, 0, keepdims=False)
        mixed = to_half(jnp.einsum('psd,rd->psr', routed.astype(jnp.float32), q_here.astype(jnp.float32)))
        factor = jnp.einsum('psr,psf->rf', mixed.astype(jnp.float32), hidden_here.astype(jnp.float32))
        gram = jnp.dot(factor, factor.T, precision=lax.Precision.HIGHEST)
        lower = jnp.linalg.cholesky(gram)
        inverse = jax.scipy.linalg.solve_triangular(lower, jnp.eye(RANK, dtype=jnp.float32), lower=True)
        ortho = jnp.dot(inverse, factor, precision=lax.Precision.HIGHEST)
        ortho_half = to_half(ortho)
        projected = to_half(jnp.einsum('psf,rf->psr', hidden_here.astype(jnp.float32), ortho_half.astype(jnp.float32)))
        q_new = jnp.einsum('psr,psd->rd', projected.astype(jnp.float32), routed.astype(jnp.float32))
        return (ortho * math.sqrt(FF), q_new)
    new_basis, q_update = lax.map(one_expert, jnp.arange(EXPERTS, dtype=jnp.int32))
    return (new_basis, q_update)
```

```python
import functools
import math

import jax
import jax.numpy as jnp
from jax import lax
from jax.experimental import pallas as pl
from jax.experimental.pallas import tpu as pltpu
from jax.sharding import PartitionSpec as P

F32, BF16 = jnp.float32, jnp.bfloat16


MESH = pl.DeviceIdType.MESH


def orthonormal(value):
    rank = value[0].shape[0]
    rows = lax.broadcasted_iota(jnp.int32, (rank, 2 * rank), 0)
    cols = lax.broadcasted_iota(jnp.int32, (rank, 2 * rank), 1)
    eye = (cols == rows + rank).astype(F32)
    tables = []
    for one in value:
        doubled = jnp.concatenate([one, jnp.zeros_like(one)], axis=0)
        gram = lax.dot_general(
            one, doubled, (((1,), (1,)), ((), ())),
            precision=lax.Precision.HIGHEST, preferred_element_type=F32,
        )
        tables.append(gram + eye)
    for k in range(rank):
        for j, table in enumerate(tables):
            row = table[k : k + 1, :]
            pivot = lax.rsqrt(row[:, k : k + 1])
            scaled = row * pivot
            column = table[:, k : k + 1] * pivot
            table = jnp.where(rows > k, table - column * scaled, table)
            tables[j] = jnp.where(rows == k, scaled, table)
    return [
        jnp.dot(
            table[:, rank:], one, precision=lax.Precision.HIGHEST, preferred_element_type=F32
        )
        for table, one in zip(tables, value)
    ]


def factor_kernel(
    n, part_ref, hidden_ref, ortho_ref, proj_ref,
    hidden, got_part, fact, got_fact, load_sem, send_sem, recv_sem,
):
    me = lax.axis_index("dp")
    experts = hidden.shape[0]
    per = experts // n
    peers = [lax.rem(me + offset, n) for offset in range(1, n)]
    loads = []
    for j in range(experts):
        load = pltpu.make_async_copy(hidden_ref.at[j], hidden.at[j], load_sem.at[j])
        load.start()
        loads.append(load)
    barrier = pltpu.get_barrier_semaphore()
    for peer in peers:
        pl.semaphore_signal(barrier, inc=1, device_id={"dp": peer}, device_id_type=MESH)
    pl.semaphore_wait(barrier, n - 1)

    def push(phase, offset, source, target):
        copy = pltpu.make_async_remote_copy(
            src_ref=source,
            dst_ref=target,
            send_sem=send_sem.at[phase, offset],
            recv_sem=recv_sem.at[phase, offset],
            device_id={"dp": peers[offset]},
            device_id_type=MESH,
        )
        copy.start()
        return copy

    sent = [push(0, o, part_ref.at[peers[o]], got_part.at[o]) for o in range(n - 1)]
    for copy in sent:
        copy.wait()
    mixed = part_ref[me].astype(F32)
    for o in range(n - 1):
        mixed = mixed + got_part[o].astype(F32)
    mixed = mixed.astype(BF16)
    for load in loads:
        load.wait()
    rank = mixed.shape[1]
    for j in range(experts):
        fact[j] = jnp.dot(mixed[j], hidden[j], preferred_element_type=F32).astype(BF16)
    sent = [
        push(1, o, fact.at[pl.ds(peers[o] * per, per)], got_fact.at[o]) for o in range(n - 1)
    ]
    for copy in sent:
        copy.wait()
    share = []
    for i in range(per):
        total = fact[me * per + i].astype(F32)
        for o in range(n - 1):
            total = total + got_fact[o, i].astype(F32)
        share.append(total)
    for i, value in enumerate(orthonormal(share)):
        ortho_ref[me * per + i] = value.astype(BF16)
    mine = ortho_ref.at[pl.ds(me * per, per)]
    sent = [push(2, o, mine, mine) for o in range(n - 1)]

    def project(group):
        for i in range(per):
            j = group * per + i
            proj_ref[me, j] = lax.dot_general(
                ortho_ref[j], hidden[j], (((1,), (1,)), ((), ())), preferred_element_type=F32
            ).astype(BF16)

    project(me)
    for o in range(n - 1):
        sent[o].wait()
        project(lax.rem(me + n - 1 - o, n))
    sent = [push(3, o, proj_ref.at[me], proj_ref.at[me]) for o in range(n - 1)]
    for copy in sent:
        copy.wait()


def factors(part, hidden, n):
    experts, slots, units = hidden.shape
    rank = part.shape[2]
    per = experts // n
    vmem = pl.BlockSpec(memory_space=pltpu.VMEM)
    return pl.pallas_call(
        functools.partial(factor_kernel, n),
        out_shape=(
            jax.ShapeDtypeStruct((experts, rank, units), BF16),
            jax.ShapeDtypeStruct((n, experts, rank, slots), BF16),
        ),
        in_specs=[vmem, pl.BlockSpec(memory_space=pl.ANY)],
        out_specs=(vmem, vmem),
        scratch_shapes=[
            pltpu.VMEM((experts, slots, units), BF16),
            pltpu.VMEM((n - 1, experts, rank, slots), BF16),
            pltpu.VMEM((experts, rank, units), BF16),
            pltpu.VMEM((n - 1, per, rank, units), BF16),
            pltpu.SemaphoreType.DMA((experts,)),
            pltpu.SemaphoreType.DMA((4, n - 1)),
            pltpu.SemaphoreType.DMA((4, n - 1)),
        ],
        compiler_params=pltpu.CompilerParams(
            collective_id=0, has_side_effects=True, vmem_limit_bytes=40 * 2**20
        ),
        name="factors",
    )(part, hidden)


def gather_kernel(
    n_expert, n_dp, x_ref, route_ref, all_ref, routes_ref,
    route_send, route_recv, own_sem, z_send, z_recv, one_send, one_recv, two_send, two_recv, core_send, core_recv,
):
    me, z = lax.axis_index("expert"), lax.axis_index("dp")
    chips = n_expert // 2
    wide = math.isqrt(chips)
    sides = (wide, chips // wide)
    core, chip = lax.rem(me, 2), me // 2
    spot = (lax.rem(chip, wide), chip // wide)
    half, cols = x_ref.shape[0] // 2, all_ref.shape[3]

    def shifted(dim, by):
        return lax.rem(spot[dim] + by + sides[dim], sides[dim])

    def block(x, y, c):
        return (y * wide + x) * 2 + c

    def neighbour(dim, by):
        moved = shifted(dim, by)
        return block(moved, spot[1], core) if dim == 0 else block(spot[0], moved, core)

    def source(dim, first, second, c):
        x, y = (first, second) if dim == 0 else (second, first)
        return block(shifted(0, -x), shifted(1, -y), c)

    barrier = pltpu.get_barrier_semaphore()
    def greet(i, carry):
        pl.semaphore_signal(barrier, inc=1, device_id=other_of(i), device_id_type=MESH)
        return carry

    def other_of(i):
        return {
            "expert": lax.rem(me + lax.rem(i, n_expert), n_expert),
            "dp": lax.rem(z + i // n_expert, n_dp),
        }

    total = n_expert * n_dp
    lax.fori_loop(1, total, greet, 0)
    pl.semaphore_wait(barrier, total - 1)

    sent = []
    mine = routes_ref.at[z, me]
    routes_ref[z, me] = route_ref[...]

    def push(src, dst, send_sem, recv_sem, device):
        copy = pltpu.make_async_remote_copy(
            src_ref=src, dst_ref=dst, send_sem=send_sem, recv_sem=recv_sem,
            device_id=device, device_id_type=MESH,
        )
        copy.start()
        sent.append(copy)
        return copy

    def columns(r):
        return x_ref.at[:, pl.ds(pl.multiple_of(r * cols, 128), cols)]

    own = pltpu.make_async_copy(columns(z), all_ref.at[me, z], own_sem)
    own.start()
    arrive_z, arrive_one, arrive_two, arrive_core = {}, {}, {}, []
    for k in range(1, n_dp):
        to = lax.rem(z + k, n_dp)
        arrive_z[k] = push(
            columns(to), all_ref.at[me, z], z_send.at[k - 1], z_recv.at[k - 1], {"dp": to}
        )

    def tell(i, carry):
        pltpu.make_async_remote_copy(
            src_ref=route_ref, dst_ref=mine, send_sem=route_send.at[i],
            recv_sem=route_recv.at[i], device_id=other_of(i), device_id_type=MESH,
        ).start()
        return carry

    lax.fori_loop(1, total, tell, 0)

    def rows(b, k, h):
        return all_ref.at[b, lax.rem(z - k + n_dp, n_dp), pl.ds(h * half, half)]

    def swap(k, h, first, second):
        part = rows(source(h, first, second, core), k, h)
        at = (h, k, first, second)
        partner = {"expert": block(spot[0], spot[1], 1 - core)}
        arrive_core.append(push(part, part, core_send.at[at], core_recv.at[at], partner))

    def onward(k, h, first):
        part = rows(source(h, first, 0, core), k, h)
        for by in range(1, sides[1 - h]):
            at = (h, k, first, by - 1)
            arrive_two[at] = push(
                part, part, two_send.at[at], two_recv.at[at], {"expert": neighbour(1 - h, by)}
            )
        swap(k, h, first, 0)

    for k in range(n_dp + 2):
        if k < n_dp:
            if k:
                arrive_z[k].wait_recv()
            else:
                own.wait()
            for h in range(2):
                part = rows(me, k, h)
                for by in range(1, sides[h]):
                    at = (h, k, by - 1)
                    arrive_one[at] = push(
                        part, part, one_send.at[at], one_recv.at[at], {"expert": neighbour(h, by)}
                    )
            for h in range(2):
                onward(k, h, 0)
        if 0 <= k - 1 < n_dp:
            for h in range(2):
                for by in range(1, sides[h]):
                    arrive_one[(h, k - 1, by - 1)].wait_recv()
                    onward(k - 1, h, by)
        if 0 <= k - 2 < n_dp:
            for h in range(2):
                for first in range(sides[h]):
                    for by in range(1, sides[1 - h]):
                        arrive_two[(h, k - 2, first, by - 1)].wait_recv()
                        swap(k - 2, h, first, by)
    def told(i, carry):
        pltpu.make_async_remote_copy(
            src_ref=route_ref, dst_ref=mine, send_sem=route_send.at[i],
            recv_sem=route_recv.at[i], device_id=other_of(i), device_id_type=MESH,
        ).wait()
        return carry

    lax.fori_loop(1, total, told, 0)
    for copy in arrive_core:
        copy.wait_recv()
    for copy in sent:
        copy.wait_send()


def gathered(grads, route):
    n_expert, n_dp = lax.axis_size("expert"), lax.axis_size("dp")
    tokens, width = grads.shape
    long = max(math.isqrt(n_expert // 2), n_expert // 2 // math.isqrt(n_expert // 2))
    dma = pltpu.SemaphoreType.DMA
    return pl.pallas_call(
        functools.partial(gather_kernel, n_expert, n_dp),
        out_shape=(
            jax.ShapeDtypeStruct((n_expert, n_dp, tokens, width // n_dp), grads.dtype),
            jax.ShapeDtypeStruct((n_dp, n_expert, *route.shape), route.dtype),
        ),
        in_specs=[pl.BlockSpec(memory_space=pltpu.VMEM)] * 2,
        out_specs=(pl.BlockSpec(memory_space=pl.ANY), pl.BlockSpec(memory_space=pltpu.VMEM)),
        scratch_shapes=[
            dma((n_expert * n_dp,)), dma((n_expert * n_dp,)), dma(()), dma((n_dp - 1,)), dma((n_dp - 1,)),
            dma((2, n_dp, long)), dma((2, n_dp, long)),
            dma((2, n_dp, long, long)), dma((2, n_dp, long, long)),
            dma((2, n_dp, long, long)), dma((2, n_dp, long, long)),
        ],
        compiler_params=pltpu.CompilerParams(
            collective_id=1, has_side_effects=True, vmem_limit_bytes=56 * 2**20
        ),
        name="gather_rows",
    )(grads, route)


def local(out_grads, expert_ids, gate_probs, hidden_acts, q_previous):
    n_expert = lax.axis_size("expert")
    n_dp = lax.axis_size("dp")
    experts, slots, units = hidden_acts.shape[1:]
    capacity = slots // n_expert
    tokens, width = out_grads.shape[1:]
    top = expert_ids.shape[2]
    rank = q_previous.shape[1]
    cols = width // n_dp
    first = lax.axis_index("expert") * experts

    route = jnp.concatenate([expert_ids[0].astype(F32), gate_probs[0]], axis=1).T
    grads, route = gathered(out_grads[0], route)
    mine = (first + jnp.arange(experts)).astype(F32)[:, None]
    ids = route[:, :, :top].transpose(2, 0, 1, 3)[:, :, :, None, :]
    weight = route[:, :, top:].transpose(2, 0, 1, 3)[:, :, :, None, :]
    hit = ids == mine
    gate = jnp.sum(jnp.where(hit, weight, 0.0), axis=0)
    chosen = jnp.any(hit, axis=0)
    earlier = (jnp.arange(tokens)[:, None] < jnp.arange(tokens)[None, :]).astype(BF16)
    place = jnp.einsum("pbjt,tu->pbju", chosen.astype(BF16), earlier, preferred_element_type=F32)
    place = jnp.where(chosen, place, -1.0)
    pick = (place[:, :, :, None, :] == jnp.arange(capacity, dtype=F32)[:, None]).astype(BF16)

    q_part = lax.dynamic_slice_in_dim(q_previous, lax.axis_index("dp") * cols, cols, 2)
    mixed = jnp.einsum("jrd,bptd->jrbpt", q_part, grads, preferred_element_type=F32)
    scale = gate.transpose(2, 1, 0, 3)
    mixed = (mixed * scale[:, None]).astype(BF16)
    part = jnp.einsum("jrbpt,pbjct->pjrbc", mixed, pick, preferred_element_type=F32).astype(BF16)
    part = part.reshape(n_dp, experts, rank, slots)
    ortho, proj = factors(part, hidden_acts[0], n_dp)
    proj = proj.reshape(n_dp, experts, rank, n_expert, capacity)
    spread = jnp.einsum("pjrbc,pbjct->jrbpt", proj, pick, preferred_element_type=F32)
    spread = (spread * scale[:, None]).astype(BF16)
    q_update = jnp.einsum("jrbpt,bptd->jrd", spread, grads, preferred_element_type=F32)
    new_basis = ortho.astype(F32) * math.sqrt(units)
    return (new_basis, q_update)


def solution(mesh):
    return jax.shard_map(
        local,
        mesh=mesh,
        in_specs=(
            P("dp", "expert", None),
            P("dp", "expert", None),
            P("dp", "expert", None),
            P("dp", "expert", None, None),
            P("expert", None, None),
        ),
        out_specs=(P("expert", None, None), P("expert", None, "dp")),
        check_vma=False,
    )
```

```python
import functools
import math

import jax
import jax.numpy as jnp
from jax import lax
from jax.experimental import pallas as pl
from jax.experimental.pallas import tpu as pltpu
from jax.sharding import PartitionSpec as P

F32, BF16 = jnp.float32, jnp.bfloat16


MESH = pl.DeviceIdType.MESH


def orthonormal(value):
    rank = value[0].shape[0]
    rows = lax.broadcasted_iota(jnp.int32, (rank, 2 * rank), 0)
    cols = lax.broadcasted_iota(jnp.int32, (rank, 2 * rank), 1)
    eye = (cols == rows + rank).astype(F32)
    tables = []
    for one in value:
        doubled = jnp.concatenate([one, jnp.zeros_like(one)], axis=0)
        gram = lax.dot_general(
            one, doubled, (((1,), (1,)), ((), ())),
            precision=lax.Precision.HIGHEST, preferred_element_type=F32,
        )
        tables.append(gram + eye)
    for k in range(rank):
        for j, table in enumerate(tables):
            row = table[k : k + 1, :]
            pivot = lax.rsqrt(row[:, k : k + 1])
            scaled = row * pivot
            column = table[:, k : k + 1] * pivot
            table = jnp.where(rows > k, table - column * scaled, table)
            tables[j] = jnp.where(rows == k, scaled, table)
    return [
        jnp.dot(
            table[:, rank:], one, precision=lax.Precision.HIGHEST, preferred_element_type=F32
        )
        for table, one in zip(tables, value)
    ]


def factor_kernel(
    n, part_ref, hidden_ref, ortho_ref, proj_ref,
    hidden, got_part, fact, got_fact, load_sem, send_sem, recv_sem,
):
    me = lax.axis_index("dp")
    experts = hidden.shape[0]
    per = experts // n
    peers = [lax.rem(me + offset, n) for offset in range(1, n)]
    loads = []
    for j in range(experts):
        load = pltpu.make_async_copy(hidden_ref.at[j], hidden.at[j], load_sem.at[j])
        load.start()
        loads.append(load)
    barrier = pltpu.get_barrier_semaphore()
    for peer in peers:
        pl.semaphore_signal(barrier, inc=1, device_id={"dp": peer}, device_id_type=MESH)
    pl.semaphore_wait(barrier, n - 1)

    def push(phase, offset, source, target):
        copy = pltpu.make_async_remote_copy(
            src_ref=source,
            dst_ref=target,
            send_sem=send_sem.at[phase, offset],
            recv_sem=recv_sem.at[phase, offset],
            device_id={"dp": peers[offset]},
            device_id_type=MESH,
        )
        copy.start()
        return copy

    sent = [push(0, o, part_ref.at[peers[o]], got_part.at[o]) for o in range(n - 1)]
    for copy in sent:
        copy.wait()
    mixed = part_ref[me].astype(F32)
    for o in range(n - 1):
        mixed = mixed + got_part[o].astype(F32)
    mixed = mixed.astype(BF16)
    for load in loads:
        load.wait()
    rank = mixed.shape[1]
    for j in range(experts):
        fact[j] = jnp.dot(mixed[j], hidden[j], preferred_element_type=F32).astype(BF16)
    sent = [
        push(1, o, fact.at[pl.ds(peers[o] * per, per)], got_fact.at[o]) for o in range(n - 1)
    ]
    for copy in sent:
        copy.wait()
    share = []
    for i in range(per):
        total = fact[me * per + i].astype(F32)
        for o in range(n - 1):
            total = total + got_fact[o, i].astype(F32)
        share.append(total)
    for i, value in enumerate(orthonormal(share)):
        ortho_ref[me * per + i] = value.astype(BF16)
    mine = ortho_ref.at[pl.ds(me * per, per)]
    sent = [push(2, o, mine, mine) for o in range(n - 1)]

    def project(group):
        for i in range(per):
            j = group * per + i
            proj_ref[me, j] = lax.dot_general(
                ortho_ref[j], hidden[j], (((1,), (1,)), ((), ())), preferred_element_type=F32
            ).astype(BF16)

    project(me)
    for o in range(n - 1):
        sent[o].wait()
        project(lax.rem(me + n - 1 - o, n))
    sent = [push(3, o, proj_ref.at[me], proj_ref.at[me]) for o in range(n - 1)]
    for copy in sent:
        copy.wait()


def factors(part, hidden, n):
    experts, slots, units = hidden.shape
    rank = part.shape[2]
    per = experts // n
    vmem = pl.BlockSpec(memory_space=pltpu.VMEM)
    return pl.pallas_call(
        functools.partial(factor_kernel, n),
        out_shape=(
            jax.ShapeDtypeStruct((experts, rank, units), BF16),
            jax.ShapeDtypeStruct((n, experts, rank, slots), BF16),
        ),
        in_specs=[vmem, pl.BlockSpec(memory_space=pl.ANY)],
        out_specs=(vmem, vmem),
        scratch_shapes=[
            pltpu.VMEM((experts, slots, units), BF16),
            pltpu.VMEM((n - 1, experts, rank, slots), BF16),
            pltpu.VMEM((experts, rank, units), BF16),
            pltpu.VMEM((n - 1, per, rank, units), BF16),
            pltpu.SemaphoreType.DMA((experts,)),
            pltpu.SemaphoreType.DMA((4, n - 1)),
            pltpu.SemaphoreType.DMA((4, n - 1)),
        ],
        compiler_params=pltpu.CompilerParams(
            collective_id=0, has_side_effects=True, vmem_limit_bytes=40 * 2**20
        ),
        name="factors",
    )(part, hidden)


def gather_kernel(
    n_expert, n_dp, x_ref, route_ref, all_ref, routes_ref,
    route_send, route_recv, own_sem, z_send, z_recv, one_send, one_recv, two_send, two_recv, core_send, core_recv,
):
    me, z = lax.axis_index("expert"), lax.axis_index("dp")
    chips = n_expert // 2
    wide = math.isqrt(chips)
    sides = (wide, chips // wide)
    core, chip = lax.rem(me, 2), me // 2
    spot = (lax.rem(chip, wide), chip // wide)
    half, cols = x_ref.shape[0] // 2, all_ref.shape[3]

    def shifted(dim, by):
        return lax.rem(spot[dim] + by + sides[dim], sides[dim])

    def block(x, y, c):
        return (y * wide + x) * 2 + c

    def neighbour(dim, by):
        moved = shifted(dim, by)
        return block(moved, spot[1], core) if dim == 0 else block(spot[0], moved, core)

    def source(dim, first, second, c):
        x, y = (first, second) if dim == 0 else (second, first)
        return block(shifted(0, -x), shifted(1, -y), c)

    barrier = pltpu.get_barrier_semaphore()
    def greet(i, carry):
        pl.semaphore_signal(barrier, inc=1, device_id=other_of(i), device_id_type=MESH)
        return carry

    def other_of(i):
        return {
            "expert": lax.rem(me + lax.rem(i, n_expert), n_expert),
            "dp": lax.rem(z + i // n_expert, n_dp),
        }

    total = n_expert * n_dp
    lax.fori_loop(1, total, greet, 0)
    pl.semaphore_wait(barrier, total - 1)

    sent = []
    mine = routes_ref.at[z, me]
    routes_ref[z, me] = route_ref[...]

    def push(src, dst, send_sem, recv_sem, device):
        copy = pltpu.make_async_remote_copy(
            src_ref=src, dst_ref=dst, send_sem=send_sem, recv_sem=recv_sem,
            device_id=device, device_id_type=MESH,
        )
        copy.start()
        sent.append(copy)
        return copy

    def columns(r):
        return x_ref.at[:, pl.ds(pl.multiple_of(r * cols, 128), cols)]

    own = pltpu.make_async_copy(columns(z), all_ref.at[me, z], own_sem)
    own.start()
    arrive_z, arrive_one, arrive_two, arrive_core = {}, {}, {}, []
    for k in range(1, n_dp):
        to = lax.rem(z + k, n_dp)
        arrive_z[k] = push(
            columns(to), all_ref.at[me, z], z_send.at[k - 1], z_recv.at[k - 1], {"dp": to}
        )

    def tell(i, carry):
        pltpu.make_async_remote_copy(
            src_ref=route_ref, dst_ref=mine, send_sem=route_send.at[i],
            recv_sem=route_recv.at[i], device_id=other_of(i), device_id_type=MESH,
        ).start()
        return carry

    lax.fori_loop(1, total, tell, 0)

    def rows(b, k, h):
        return all_ref.at[b, lax.rem(z - k + n_dp, n_dp), pl.ds(h * half, half)]

    def swap(k, h, first, second):
        part = rows(source(h, first, second, core), k, h)
        at = (h, k, first, second)
        partner = {"expert": block(spot[0], spot[1], 1 - core)}
        arrive_core.append(push(part, part, core_send.at[at], core_recv.at[at], partner))

    def onward(k, h, first):
        part = rows(source(h, first, 0, core), k, h)
        for by in range(1, sides[1 - h]):
            at = (h, k, first, by - 1)
            arrive_two[at] = push(
                part, part, two_send.at[at], two_recv.at[at], {"expert": neighbour(1 - h, by)}
            )
        swap(k, h, first, 0)

    for k in range(n_dp + 2):
        if k < n_dp:
            if k:
                arrive_z[k].wait_recv()
            else:
                own.wait()
            for h in range(2):
                part = rows(me, k, h)
                for by in range(1, sides[h]):
                    at = (h, k, by - 1)
                    arrive_one[at] = push(
                        part, part, one_send.at[at], one_recv.at[at], {"expert": neighbour(h, by)}
                    )
            for h in range(2):
                onward(k, h, 0)
        if 0 <= k - 1 < n_dp:
            for h in range(2):
                for by in range(1, sides[h]):
                    arrive_one[(h, k - 1, by - 1)].wait_recv()
                    onward(k - 1, h, by)
        if 0 <= k - 2 < n_dp:
            for h in range(2):
                for first in range(sides[h]):
                    for by in range(1, sides[1 - h]):
                        arrive_two[(h, k - 2, first, by - 1)].wait_recv()
                        swap(k - 2, h, first, by)
    def told(i, carry):
        pltpu.make_async_remote_copy(
            src_ref=route_ref, dst_ref=mine, send_sem=route_send.at[i],
            recv_sem=route_recv.at[i], device_id=other_of(i), device_id_type=MESH,
        ).wait()
        return carry

    lax.fori_loop(1, total, told, 0)
    for copy in arrive_core:
        copy.wait_recv()
    for copy in sent:
        copy.wait_send()


def gathered(grads, route):
    n_expert, n_dp = lax.axis_size("expert"), lax.axis_size("dp")
    tokens, width = grads.shape
    long = max(math.isqrt(n_expert // 2), n_expert // 2 // math.isqrt(n_expert // 2))
    dma = pltpu.SemaphoreType.DMA
    return pl.pallas_call(
        functools.partial(gather_kernel, n_expert, n_dp),
        out_shape=(
            jax.ShapeDtypeStruct((n_expert, n_dp, tokens, width // n_dp), grads.dtype),
            jax.ShapeDtypeStruct((n_dp, n_expert, *route.shape), route.dtype),
        ),
        in_specs=[pl.BlockSpec(memory_space=pltpu.VMEM)] * 2,
        out_specs=(pl.BlockSpec(memory_space=pl.ANY), pl.BlockSpec(memory_space=pltpu.VMEM)),
        scratch_shapes=[
            dma((n_expert * n_dp,)), dma((n_expert * n_dp,)), dma(()), dma((n_dp - 1,)), dma((n_dp - 1,)),
            dma((2, n_dp, long)), dma((2, n_dp, long)),
            dma((2, n_dp, long, long)), dma((2, n_dp, long, long)),
            dma((2, n_dp, long, long)), dma((2, n_dp, long, long)),
        ],
        compiler_params=pltpu.CompilerParams(
            collective_id=1, has_side_effects=True, vmem_limit_bytes=56 * 2**20
        ),
        name="gather_rows",
    )(grads, route)


def fused_kernel(
    n_expert, n_dp, grads_ref, route_ref, hidden_ref, q_ref, ortho_ref, upd_ref,
    rep, bulk, hid, qv, routes, gate, pick, mixed, fact, got_up, got_cross, tot, gram, proj, spr,
    load_sem, route_send, route_recv, far_send, far_recv, z_send, z_recv,
    one_send, one_recv, two_send, two_recv, core_send, core_recv,
    ring_send, ring_recv, proj_send, proj_recv,
):
    me, z = lax.axis_index("expert"), lax.axis_index("dp")
    chips = n_expert // 2
    wide = math.isqrt(chips)
    sides = (wide, chips // wide)
    core, chip = lax.rem(me, 2), me // 2
    spot = (lax.rem(chip, wide), chip // wide)
    tokens, cols = rep.shape[2:]
    half = tokens // 2
    experts, slots, units = hid.shape
    rank = fact.shape[1]
    cap = slots // n_expert
    top = routes.shape[2] // 2
    group = mixed.shape[0]
    span = n_expert // group

    def shifted(dim, by):
        return lax.rem(spot[dim] + by + sides[dim], sides[dim])

    def block(x, y, c):
        return (y * wide + x) * 2 + c

    def neighbour(dim, by):
        moved = shifted(dim, by)
        return block(moved, spot[1], core) if dim == 0 else block(spot[0], moved, core)

    def source(dim, first, second, c):
        x, y = (first, second) if dim == 0 else (second, first)
        return block(shifted(0, -x), shifted(1, -y), c)

    def beside(i):
        return {"expert": lax.rem(me + i, n_expert)}

    def along(k):
        return {"dp": lax.rem(z + k, n_dp)}

    loads = []

    def load(src, dst):
        copy = pltpu.make_async_copy(src, dst, load_sem.at[len(loads)])
        copy.start()
        loads.append(copy)

    for k in range(n_dp):
        load(grads_ref.at[:, pl.ds(k * cols, cols)], rep.at[k, me])
    for k in range(n_dp):
        load(q_ref.at[:, pl.ds(k * cols, cols)], qv.at[k])
    for j in range(experts):
        load(hidden_ref.at[j], hid.at[j])

    barrier = pltpu.get_barrier_semaphore()
    greeted = [along(k) for k in range(1, n_dp)] + [beside(i) for i in range(1, n_expert)]
    for peer in greeted:
        pl.semaphore_signal(barrier, inc=1, device_id=peer, device_id_type=MESH)
    routes[0, me] = route_ref[...]
    pl.semaphore_wait(barrier, len(greeted))

    sent = []

    def push(src, dst, send_sem, recv_sem, device):
        copy = pltpu.make_async_remote_copy(
            src_ref=src, dst_ref=dst, send_sem=send_sem, recv_sem=recv_sem,
            device_id=device, device_id_type=MESH,
        )
        copy.start()
        sent.append(copy)
        return copy

    told, told_far, arrive_z = {}, {}, {}
    for i in range(1, n_expert):
        told[0, i] = push(
            route_ref, routes.at[0, me], route_send.at[0, i], route_recv.at[0, i], beside(i)
        )
    for k in range(1, n_dp):
        told_far[k] = push(route_ref, routes.at[k, me], far_send.at[k], far_recv.at[k], along(k))

    arrive_one, arrive_two, arrive_core = {}, {}, {}

    def rows(b, k, h):
        own = rep.at[k, b] if k < n_dp else bulk.at[k - n_dp, b]
        return own.at[pl.ds(h * half, half)]

    def swap(k, h, first, second):
        part = rows(source(h, first, second, core), k, h)
        at = (h, k, first, second)
        partner = {"expert": block(spot[0], spot[1], 1 - core)}
        arrive_core[at] = push(part, part, core_send.at[at], core_recv.at[at], partner)

    def onward(k, h, first):
        part = rows(source(h, first, 0, core), k, h)
        for by in range(1, sides[1 - h]):
            at = (h, k, first, by - 1)
            arrive_two[at] = push(
                part, part, two_send.at[at], two_recv.at[at], {"expert": neighbour(1 - h, by)}
            )
        swap(k, h, first, 0)

    def begin(k):
        for h in range(2):
            part = rows(me, k, h)
            for by in range(1, sides[h]):
                at = (h, k, by - 1)
                arrive_one[at] = push(
                    part, part, one_send.at[at], one_recv.at[at], {"expert": neighbour(h, by)}
                )
        for h in range(2):
            onward(k, h, 0)

    def forward(k):
        for h in range(2):
            for by in range(1, sides[h]):
                arrive_one[h, k, by - 1].wait_recv()
                onward(k, h, by)

    def second(k):
        for h in range(2):
            for first in range(sides[h]):
                for by in range(1, sides[1 - h]):
                    arrive_two[h, k, first, by - 1].wait_recv()
                    swap(k, h, first, by)

    def landed(k):
        for at, copy in arrive_core.items():
            if at[1] == k:
                copy.wait_recv()

    def accumulate(k):
        for p in range(group):
            piece = rep[k, p * span : (p + 1) * span].reshape(span * tokens, cols)
            value = lax.dot_general(
                qv[k], piece, (((1,), (1,)), ((), ())), preferred_element_type=F32
            )
            mixed[p] = value if k == 0 else mixed[p] + value

    def place_tokens(k):
        for i in range(1, n_expert):
            told[k, i].wait_recv()
        ours = lax.broadcasted_iota(jnp.int32, (experts, tokens), 0) + me * experts
        ours = ours.astype(F32)
        gates, hits = [], []
        for b in range(n_expert):
            table = routes[k, b]
            value = jnp.zeros((experts, tokens), F32)
            hit = jnp.zeros((experts, tokens), F32)
            for t in range(top):
                same = table[t : t + 1, :] == ours
                value = jnp.where(same, table[top + t : top + t + 1, :], value)
                hit = jnp.where(same, 1.0, hit)
            gates.append(value)
            hits.append(hit)
        gate[k] = jnp.concatenate(gates, axis=1)
        hits = jnp.concatenate(hits, axis=0)
        before = lax.broadcasted_iota(jnp.int32, (tokens, tokens), 0)
        after = lax.broadcasted_iota(jnp.int32, (tokens, tokens), 1)
        earlier = jnp.where(before < after, 1.0, 0.0).astype(BF16)
        count = jnp.dot(hits.astype(BF16), earlier, preferred_element_type=F32)
        count = jnp.where(hits > 0.5, count, -float(slots))
        keys = [
            count[b * experts : (b + 1) * experts] + float(b * cap) for b in range(n_expert)
        ]
        key = jnp.concatenate(keys, axis=1).astype(jnp.int32)
        level = lax.broadcasted_iota(jnp.int32, (slots, n_expert * tokens), 0)
        for j in range(experts):
            pick[k, j] = jnp.where(level == key[j : j + 1, :], 1.0, 0.0).astype(BF16)

    for k in range(n_dp):
        loads[k].wait()
    for k in range(1, n_dp):
        to = lax.rem(z + k, n_dp)
        arrive_z[k] = push(
            rep.at[to, me], bulk.at[k - 1, me], z_send.at[k], z_recv.at[k], along(k)
        )
    for k in range(n_dp + 3):
        if k < n_dp:
            begin(k)
        if 0 <= k - 1 < n_dp:
            forward(k - 1)
        if k == 0:
            place_tokens(0)
        if k == n_dp:
            for r in range(1, n_dp):
                told_far[r].wait_recv()
                for i in range(1, n_expert):
                    told[r, i] = push(
                        routes.at[r, me], routes.at[r, me],
                        route_send.at[r, i], route_recv.at[r, i], beside(i),
                    )
            for r in range(1, n_dp):
                arrive_z[r].wait_recv()
                begin(n_dp + r - 1)
        if 0 <= k - 2 < n_dp:
            second(k - 2)
        if 0 <= k - 3 < n_dp:
            loads[n_dp + k - 3].wait()
            landed(k - 3)
            accumulate(k - 3)
    for copy in loads[2 * n_dp :]:
        copy.wait()

    mate = z + 1 - 2 * lax.rem(z, 2)
    cross = n_dp - 1 - z
    inner = jnp.logical_or(z == 1, z == 2)

    def hop(kind, j, src, dst, to):
        return pltpu.make_async_remote_copy(
            src_ref=src.at[j], dst_ref=dst.at[j],
            send_sem=ring_send.at[kind, j], recv_sem=ring_recv.at[kind, j],
            device_id={"dp": to}, device_id_type=MESH,
        )

    def up(j):
        return hop(0, j, fact, got_up, mate)

    def over(j):
        return hop(1, j, fact, got_cross, cross)

    def down(j):
        return hop(2, j, tot, tot, mate)

    for j in range(experts):
        value = jnp.concatenate([mixed[p, j * rank : (j + 1) * rank] for p in range(group)], axis=1)
        value = (value * gate[0, j : j + 1, :]).astype(BF16)
        value = lax.dot_general(
            value, pick[0, j], (((1,), (1,)), ((), ())), preferred_element_type=F32
        ).astype(BF16)
        fact[j] = jnp.dot(value, hid[j], preferred_element_type=F32).astype(BF16)

        @pl.when(jnp.logical_not(inner))
        def _():
            up(j).start()

    ahead = 2
    others = list(range(1, n_dp))
    for step in range(experts + ahead):
        if step < experts:

            @pl.when(inner)
            def _():
                up(step).wait_recv()
                fact[step] = (fact[step].astype(F32) + got_up[step].astype(F32)).astype(BF16)
                over(step).start()

        if step >= ahead:
            j = step - ahead

            @pl.when(inner)
            def _():
                over(j).wait_recv()
                tot[j] = (fact[j].astype(F32) + got_cross[j].astype(F32)).astype(BF16)
                down(j).start()

        if 1 <= step <= len(others):
            place_tokens(others[step - 1])
    for r in range(1, n_dp):
        forward(n_dp + r - 1)

    shape = (rank, 2 * rank)
    eye = lax.broadcasted_iota(jnp.int32, shape, 1) == lax.broadcasted_iota(jnp.int32, shape, 0) + rank
    eye = jnp.where(eye, 1.0, 0.0)
    for j in range(experts):

        @pl.when(jnp.logical_not(inner))
        def _():
            down(j).wait_recv()

        one = tot[j]
        doubled = jnp.concatenate([one, jnp.zeros_like(one)], axis=0)
        gram[j] = eye + lax.dot_general(
            one, doubled, (((1,), (1,)), ((), ())), preferred_element_type=F32
        )

    table = [gram[:, k, :] for k in range(rank)]
    for k in range(rank):
        row = table[k]
        scaled = row / row[:, k : k + 1]
        for i in range(k + 1, rank):
            table[i] = table[i] - row[:, i : i + 1] * scaled
        table[k] = row * lax.rsqrt(row[:, k : k + 1])
    for k in range(rank):
        gram[:, k, :] = table[k]

    batch = experts // 2
    arrive_proj = {}
    for j in range(experts):
        inverse = gram[j][:, rank:]
        high = inverse.astype(BF16)
        low = (inverse - high.astype(F32)).astype(BF16)
        one = tot[j]
        value = jnp.dot(high, one, preferred_element_type=F32)
        value = (value + jnp.dot(low, one, preferred_element_type=F32)).astype(BF16)
        ortho_ref[j] = value
        proj[0, j // 2, :, (j % 2) * slots : (j % 2 + 1) * slots] = lax.dot_general(
            value, hid[j], (((1,), (1,)), ((), ())), preferred_element_type=F32
        ).astype(BF16)
        if (j + 1) % batch == 0:
            g = j // batch
            part = pl.ds(g * batch // 2, batch // 2)
            for k in range(1, n_dp):
                arrive_proj[k, g] = push(
                    proj.at[0, part], proj.at[k, part],
                    proj_send.at[k, g], proj_recv.at[k, g], along(k),
                )

    def update(k):
        if k:
            for g in range(2):
                arrive_proj[k, g].wait_recv()
        for j in range(experts):
            value = jnp.dot(
                proj[k, j // 2, :, (j % 2) * slots : (j % 2 + 1) * slots], pick[k, j],
                preferred_element_type=F32,
            )
            spr[j * rank : (j + 1) * rank] = (value * gate[k, j : j + 1, :]).astype(BF16)
        if k:
            landed(n_dp + k - 1)
        own = bulk.at[k - 1] if k else rep.at[z]

        def tile(c, carry):
            at = pl.ds(pl.multiple_of(c * 256, 256), 256)
            right = own[:, :, at].reshape(n_expert * tokens, 256)
            value = jnp.dot(spr[...], right, preferred_element_type=F32)
            upd_ref[:, at] = upd_ref[:, at] + value if k else value
            return carry

        lax.fori_loop(0, cols // 256, tile, 0)

    update(0)
    for r in range(1, n_dp):
        second(n_dp + r - 1)
    for r in range(1, n_dp):
        update(r)
    for j in range(experts):

        @pl.when(inner)
        def _():
            over(j).wait_send()
            down(j).wait_send()

        @pl.when(jnp.logical_not(inner))
        def _():
            up(j).wait_send()

    for copy in sent:
        copy.wait_send()


def fused_buffers(n_expert, n_dp, tokens, width, experts, slots, units, rank, top):
    cols = width // n_dp
    return [
        ((n_dp, n_expert, tokens, cols), BF16),
        ((n_dp - 1, n_expert, tokens, cols), BF16),
        ((experts, slots, units), BF16),
        ((n_dp, experts * rank, cols), BF16),
        ((n_dp, n_expert, 2 * top, tokens), F32),
        ((n_dp, experts, n_expert * tokens), F32),
        ((n_dp, experts, slots, n_expert * tokens), BF16),
        ((n_expert // 2, experts * rank, 2 * tokens), F32),
        ((experts, rank, units), BF16),
        ((experts, rank, units), BF16),
        ((experts, rank, units), BF16),
        ((experts, rank, units), BF16),
        ((experts, rank, 2 * rank), F32),
        ((n_dp, experts // 2, rank, 2 * slots), BF16),
        ((experts * rank, n_expert * tokens), BF16),
    ]


def fused(grads, route, hidden, q, buffers):
    n_expert, n_dp = lax.axis_size("expert"), lax.axis_size("dp")
    experts, slots, units = hidden.shape
    rank = q.shape[0] // experts
    cols = q.shape[1] // n_dp
    chips = n_expert // 2
    long = max(math.isqrt(chips), chips // math.isqrt(chips))
    tags = 2 * n_dp - 1
    dma = pltpu.SemaphoreType.DMA
    vmem = pl.BlockSpec(memory_space=pltpu.VMEM)
    anywhere = pl.BlockSpec(memory_space=pl.ANY)
    return pl.pallas_call(
        functools.partial(fused_kernel, n_expert, n_dp),
        out_shape=(
            jax.ShapeDtypeStruct((experts, rank, units), BF16),
            jax.ShapeDtypeStruct((experts * rank, cols), F32),
        ),
        in_specs=[anywhere, vmem, anywhere, anywhere],
        out_specs=(vmem, vmem),
        scratch_shapes=[pltpu.VMEM(*b) for b in buffers] + [
            dma((2 * n_dp + experts,)),
            dma((n_dp, n_expert)), dma((n_dp, n_expert)), dma((n_dp,)), dma((n_dp,)),
            dma((n_dp,)), dma((n_dp,)),
            dma((2, tags, long)), dma((2, tags, long)),
            dma((2, tags, long, long)), dma((2, tags, long, long)),
            dma((2, tags, long, long)), dma((2, tags, long, long)),
            dma((3, experts)), dma((3, experts)), dma((n_dp, 2)), dma((n_dp, 2)),
        ],
        compiler_params=pltpu.CompilerParams(
            collective_id=2, has_side_effects=True, vmem_limit_bytes=67043328
        ),
        name="fused",
    )(grads, route, hidden, q)


def local(out_grads, expert_ids, gate_probs, hidden_acts, q_previous):
    n_expert, n_dp = lax.axis_size("expert"), lax.axis_size("dp")
    experts, slots, units = hidden_acts.shape[1:]
    tokens, width = out_grads.shape[1:]
    rank = q_previous.shape[1]
    cols = width // n_dp
    buffers = fused_buffers(
        n_expert, n_dp, tokens, width, experts, slots, units, rank, expert_ids.shape[2]
    )
    held = sum(math.prod(shape) * jnp.dtype(kind).itemsize for shape, kind in buffers)
    held += experts * rank * (4 * cols + 2 * units)
    if n_dp != 4 or held > 60 * 2**20:
        return spacious(out_grads, expert_ids, gate_probs, hidden_acts, q_previous)
    route = jnp.concatenate([expert_ids[0].astype(F32), gate_probs[0]], axis=1).T
    q = q_previous.reshape(experts * rank, width)
    ortho, update = fused(out_grads[0], route, hidden_acts[0], q, buffers)
    return (ortho.astype(F32) * math.sqrt(units), update.reshape(experts, rank, cols))


def spacious(out_grads, expert_ids, gate_probs, hidden_acts, q_previous):
    n_expert = lax.axis_size("expert")
    n_dp = lax.axis_size("dp")
    experts, slots, units = hidden_acts.shape[1:]
    capacity = slots // n_expert
    tokens, width = out_grads.shape[1:]
    top = expert_ids.shape[2]
    rank = q_previous.shape[1]
    cols = width // n_dp
    first = lax.axis_index("expert") * experts

    route = jnp.concatenate([expert_ids[0].astype(F32), gate_probs[0]], axis=1).T
    grads, route = gathered(out_grads[0], route)
    mine = (first + jnp.arange(experts)).astype(F32)[:, None]
    ids = route[:, :, :top].transpose(2, 0, 1, 3)[:, :, :, None, :]
    weight = route[:, :, top:].transpose(2, 0, 1, 3)[:, :, :, None, :]
    hit = ids == mine
    gate = jnp.sum(jnp.where(hit, weight, 0.0), axis=0)
    chosen = jnp.any(hit, axis=0)
    earlier = (jnp.arange(tokens)[:, None] < jnp.arange(tokens)[None, :]).astype(BF16)
    place = jnp.einsum("pbjt,tu->pbju", chosen.astype(BF16), earlier, preferred_element_type=F32)
    place = jnp.where(chosen, place, -1.0)
    pick = (place[:, :, :, None, :] == jnp.arange(capacity, dtype=F32)[:, None]).astype(BF16)

    q_part = lax.dynamic_slice_in_dim(q_previous, lax.axis_index("dp") * cols, cols, 2)
    mixed = jnp.einsum("jrd,bptd->jrbpt", q_part, grads, preferred_element_type=F32)
    scale = gate.transpose(2, 1, 0, 3)
    mixed = (mixed * scale[:, None]).astype(BF16)
    part = jnp.einsum("jrbpt,pbjct->pjrbc", mixed, pick, preferred_element_type=F32).astype(BF16)
    part = part.reshape(n_dp, experts, rank, slots)
    ortho, proj = factors(part, hidden_acts[0], n_dp)
    proj = proj.reshape(n_dp, experts, rank, n_expert, capacity)
    spread = jnp.einsum("pjrbc,pbjct->jrbpt", proj, pick, preferred_element_type=F32)
    spread = (spread * scale[:, None]).astype(BF16)
    q_update = jnp.einsum("jrbpt,bptd->jrd", spread, grads, preferred_element_type=F32)
    new_basis = ortho.astype(F32) * math.sqrt(units)
    return (new_basis, q_update)


def solution(mesh):
    return jax.shard_map(
        local,
        mesh=mesh,
        in_specs=(
            P("dp", "expert", None),
            P("dp", "expert", None),
            P("dp", "expert", None),
            P("dp", "expert", None, None),
            P("expert", None, None),
        ),
        out_specs=(P("expert", None, None), P("expert", None, "dp")),
        check_vma=False,
    )
```

```python
import functools
import math

import jax
import jax.numpy as jnp
from jax import lax
from jax.experimental import pallas as pl
from jax.experimental.pallas import tpu as pltpu
from jax.sharding import PartitionSpec as P

F32, BF16 = jnp.float32, jnp.bfloat16


MESH = pl.DeviceIdType.MESH


def orthonormal(value):
    rank = value[0].shape[0]
    rows = lax.broadcasted_iota(jnp.int32, (rank, 2 * rank), 0)
    cols = lax.broadcasted_iota(jnp.int32, (rank, 2 * rank), 1)
    eye = (cols == rows + rank).astype(F32)
    tables = []
    for one in value:
        doubled = jnp.concatenate([one, jnp.zeros_like(one)], axis=0)
        gram = lax.dot_general(
            one, doubled, (((1,), (1,)), ((), ())),
            precision=lax.Precision.HIGHEST, preferred_element_type=F32,
        )
        tables.append(gram + eye)
    for k in range(rank):
        for j, table in enumerate(tables):
            row = table[k : k + 1, :]
            pivot = lax.rsqrt(row[:, k : k + 1])
            scaled = row * pivot
            column = table[:, k : k + 1] * pivot
            table = jnp.where(rows > k, table - column * scaled, table)
            tables[j] = jnp.where(rows == k, scaled, table)
    return [
        jnp.dot(
            table[:, rank:], one, precision=lax.Precision.HIGHEST, preferred_element_type=F32
        )
        for table, one in zip(tables, value)
    ]


def factor_kernel(
    n, part_ref, hidden_ref, ortho_ref, proj_ref,
    hidden, got_part, fact, got_fact, load_sem, send_sem, recv_sem,
):
    me = lax.axis_index("dp")
    experts = hidden.shape[0]
    per = experts // n
    peers = [lax.rem(me + offset, n) for offset in range(1, n)]
    loads = []
    for j in range(experts):
        load = pltpu.make_async_copy(hidden_ref.at[j], hidden.at[j], load_sem.at[j])
        load.start()
        loads.append(load)
    barrier = pltpu.get_barrier_semaphore()
    for peer in peers:
        pl.semaphore_signal(barrier, inc=1, device_id={"dp": peer}, device_id_type=MESH)
    pl.semaphore_wait(barrier, n - 1)

    def push(phase, offset, source, target):
        copy = pltpu.make_async_remote_copy(
            src_ref=source,
            dst_ref=target,
            send_sem=send_sem.at[phase, offset],
            recv_sem=recv_sem.at[phase, offset],
            device_id={"dp": peers[offset]},
            device_id_type=MESH,
        )
        copy.start()
        return copy

    sent = [push(0, o, part_ref.at[peers[o]], got_part.at[o]) for o in range(n - 1)]
    for copy in sent:
        copy.wait()
    mixed = part_ref[me].astype(F32)
    for o in range(n - 1):
        mixed = mixed + got_part[o].astype(F32)
    mixed = mixed.astype(BF16)
    for load in loads:
        load.wait()
    rank = mixed.shape[1]
    for j in range(experts):
        fact[j] = jnp.dot(mixed[j], hidden[j], preferred_element_type=F32).astype(BF16)
    sent = [
        push(1, o, fact.at[pl.ds(peers[o] * per, per)], got_fact.at[o]) for o in range(n - 1)
    ]
    for copy in sent:
        copy.wait()
    share = []
    for i in range(per):
        total = fact[me * per + i].astype(F32)
        for o in range(n - 1):
            total = total + got_fact[o, i].astype(F32)
        share.append(total)
    for i, value in enumerate(orthonormal(share)):
        ortho_ref[me * per + i] = value.astype(BF16)
    mine = ortho_ref.at[pl.ds(me * per, per)]
    sent = [push(2, o, mine, mine) for o in range(n - 1)]

    def project(group):
        for i in range(per):
            j = group * per + i
            proj_ref[me, j] = lax.dot_general(
                ortho_ref[j], hidden[j], (((1,), (1,)), ((), ())), preferred_element_type=F32
            ).astype(BF16)

    project(me)
    for o in range(n - 1):
        sent[o].wait()
        project(lax.rem(me + n - 1 - o, n))
    sent = [push(3, o, proj_ref.at[me], proj_ref.at[me]) for o in range(n - 1)]
    for copy in sent:
        copy.wait()


def factors(part, hidden, n):
    experts, slots, units = hidden.shape
    rank = part.shape[2]
    per = experts // n
    vmem = pl.BlockSpec(memory_space=pltpu.VMEM)
    return pl.pallas_call(
        functools.partial(factor_kernel, n),
        out_shape=(
            jax.ShapeDtypeStruct((experts, rank, units), BF16),
            jax.ShapeDtypeStruct((n, experts, rank, slots), BF16),
        ),
        in_specs=[vmem, pl.BlockSpec(memory_space=pl.ANY)],
        out_specs=(vmem, vmem),
        scratch_shapes=[
            pltpu.VMEM((experts, slots, units), BF16),
            pltpu.VMEM((n - 1, experts, rank, slots), BF16),
            pltpu.VMEM((experts, rank, units), BF16),
            pltpu.VMEM((n - 1, per, rank, units), BF16),
            pltpu.SemaphoreType.DMA((experts,)),
            pltpu.SemaphoreType.DMA((4, n - 1)),
            pltpu.SemaphoreType.DMA((4, n - 1)),
        ],
        compiler_params=pltpu.CompilerParams(
            collective_id=0, has_side_effects=True, vmem_limit_bytes=40 * 2**20
        ),
        name="factors",
    )(part, hidden)


def gather_kernel(
    n_expert, n_dp, x_ref, route_ref, all_ref, routes_ref,
    route_send, route_recv, own_sem, z_send, z_recv, one_send, one_recv, two_send, two_recv, core_send, core_recv,
):
    me, z = lax.axis_index("expert"), lax.axis_index("dp")
    chips = n_expert // 2
    wide = math.isqrt(chips)
    sides = (wide, chips // wide)
    core, chip = lax.rem(me, 2), me // 2
    spot = (lax.rem(chip, wide), chip // wide)
    half, cols = x_ref.shape[0] // 2, all_ref.shape[3]

    def shifted(dim, by):
        return lax.rem(spot[dim] + by + sides[dim], sides[dim])

    def block(x, y, c):
        return (y * wide + x) * 2 + c

    def neighbour(dim, by):
        moved = shifted(dim, by)
        return block(moved, spot[1], core) if dim == 0 else block(spot[0], moved, core)

    def source(dim, first, second, c):
        x, y = (first, second) if dim == 0 else (second, first)
        return block(shifted(0, -x), shifted(1, -y), c)

    barrier = pltpu.get_barrier_semaphore()
    def greet(i, carry):
        pl.semaphore_signal(barrier, inc=1, device_id=other_of(i), device_id_type=MESH)
        return carry

    def other_of(i):
        return {
            "expert": lax.rem(me + lax.rem(i, n_expert), n_expert),
            "dp": lax.rem(z + i // n_expert, n_dp),
        }

    total = n_expert * n_dp
    lax.fori_loop(1, total, greet, 0)
    pl.semaphore_wait(barrier, total - 1)

    sent = []
    mine = routes_ref.at[z, me]
    routes_ref[z, me] = route_ref[...]

    def push(src, dst, send_sem, recv_sem, device):
        copy = pltpu.make_async_remote_copy(
            src_ref=src, dst_ref=dst, send_sem=send_sem, recv_sem=recv_sem,
            device_id=device, device_id_type=MESH,
        )
        copy.start()
        sent.append(copy)
        return copy

    def columns(r):
        return x_ref.at[:, pl.ds(pl.multiple_of(r * cols, 128), cols)]

    own = pltpu.make_async_copy(columns(z), all_ref.at[me, z], own_sem)
    own.start()
    arrive_z, arrive_one, arrive_two, arrive_core = {}, {}, {}, []
    for k in range(1, n_dp):
        to = lax.rem(z + k, n_dp)
        arrive_z[k] = push(
            columns(to), all_ref.at[me, z], z_send.at[k - 1], z_recv.at[k - 1], {"dp": to}
        )

    def tell(i, carry):
        pltpu.make_async_remote_copy(
            src_ref=route_ref, dst_ref=mine, send_sem=route_send.at[i],
            recv_sem=route_recv.at[i], device_id=other_of(i), device_id_type=MESH,
        ).start()
        return carry

    lax.fori_loop(1, total, tell, 0)

    def rows(b, k, h):
        return all_ref.at[b, lax.rem(z - k + n_dp, n_dp), pl.ds(h * half, half)]

    def swap(k, h, first, second):
        part = rows(source(h, first, second, core), k, h)
        at = (h, k, first, second)
        partner = {"expert": block(spot[0], spot[1], 1 - core)}
        arrive_core.append(push(part, part, core_send.at[at], core_recv.at[at], partner))

    def onward(k, h, first):
        part = rows(source(h, first, 0, core), k, h)
        for by in range(1, sides[1 - h]):
            at = (h, k, first, by - 1)
            arrive_two[at] = push(
                part, part, two_send.at[at], two_recv.at[at], {"expert": neighbour(1 - h, by)}
            )
        swap(k, h, first, 0)

    for k in range(n_dp + 2):
        if k < n_dp:
            if k:
                arrive_z[k].wait_recv()
            else:
                own.wait()
            for h in range(2):
                part = rows(me, k, h)
                for by in range(1, sides[h]):
                    at = (h, k, by - 1)
                    arrive_one[at] = push(
                        part, part, one_send.at[at], one_recv.at[at], {"expert": neighbour(h, by)}
                    )
            for h in range(2):
                onward(k, h, 0)
        if 0 <= k - 1 < n_dp:
            for h in range(2):
                for by in range(1, sides[h]):
                    arrive_one[(h, k - 1, by - 1)].wait_recv()
                    onward(k - 1, h, by)
        if 0 <= k - 2 < n_dp:
            for h in range(2):
                for first in range(sides[h]):
                    for by in range(1, sides[1 - h]):
                        arrive_two[(h, k - 2, first, by - 1)].wait_recv()
                        swap(k - 2, h, first, by)
    def told(i, carry):
        pltpu.make_async_remote_copy(
            src_ref=route_ref, dst_ref=mine, send_sem=route_send.at[i],
            recv_sem=route_recv.at[i], device_id=other_of(i), device_id_type=MESH,
        ).wait()
        return carry

    lax.fori_loop(1, total, told, 0)
    for copy in arrive_core:
        copy.wait_recv()
    for copy in sent:
        copy.wait_send()


def gathered(grads, route):
    n_expert, n_dp = lax.axis_size("expert"), lax.axis_size("dp")
    tokens, width = grads.shape
    long = max(math.isqrt(n_expert // 2), n_expert // 2 // math.isqrt(n_expert // 2))
    dma = pltpu.SemaphoreType.DMA
    return pl.pallas_call(
        functools.partial(gather_kernel, n_expert, n_dp),
        out_shape=(
            jax.ShapeDtypeStruct((n_expert, n_dp, tokens, width // n_dp), grads.dtype),
            jax.ShapeDtypeStruct((n_dp, n_expert, *route.shape), route.dtype),
        ),
        in_specs=[pl.BlockSpec(memory_space=pltpu.VMEM)] * 2,
        out_specs=(pl.BlockSpec(memory_space=pl.ANY), pl.BlockSpec(memory_space=pltpu.VMEM)),
        scratch_shapes=[
            dma((n_expert * n_dp,)), dma((n_expert * n_dp,)), dma(()), dma((n_dp - 1,)), dma((n_dp - 1,)),
            dma((2, n_dp, long)), dma((2, n_dp, long)),
            dma((2, n_dp, long, long)), dma((2, n_dp, long, long)),
            dma((2, n_dp, long, long)), dma((2, n_dp, long, long)),
        ],
        compiler_params=pltpu.CompilerParams(
            collective_id=1, has_side_effects=True, vmem_limit_bytes=56 * 2**20
        ),
        name="gather_rows",
    )(grads, route)


def fused_kernel(
    n_expert, n_dp, grads_ref, ids_ref, probs_ref, hidden_ref, q_ref, basis_ref, upd_ref,
    rep, bulk, hid, qv, routes, gate, pick, mixed, fact, got_up, got_cross, tot, gram, proj, spr,
    basis, upd, out_sem, load_sem, route_send, route_recv, far_send, far_recv, z_send, z_recv,
    one_send, one_recv, two_send, two_recv, core_send, core_recv,
    ring_send, ring_recv, proj_send, proj_recv,
):
    me, z = lax.axis_index("expert"), lax.axis_index("dp")
    chips = n_expert // 2
    wide = math.isqrt(chips)
    sides = (wide, chips // wide)
    core, chip = lax.rem(me, 2), me // 2
    spot = (lax.rem(chip, wide), chip // wide)
    tokens, cols = rep.shape[2:]
    half = tokens // 2
    experts, slots, units = hid.shape
    rank = 2 * fact.shape[1]
    cap = slots // n_expert
    top = routes.shape[2] // 2
    group = mixed.shape[0]
    span = n_expert // group

    def shifted(dim, by):
        return lax.rem(spot[dim] + by + sides[dim], sides[dim])

    def block(x, y, c):
        return (y * wide + x) * 2 + c

    def neighbour(dim, by):
        moved = shifted(dim, by)
        return block(moved, spot[1], core) if dim == 0 else block(spot[0], moved, core)

    def source(dim, first, second, c):
        x, y = (first, second) if dim == 0 else (second, first)
        return block(shifted(0, -x), shifted(1, -y), c)

    def beside(i):
        return {"expert": lax.rem(me + i, n_expert)}

    def along(k):
        return {"dp": lax.rem(z + k, n_dp)}

    loads = []

    def load(src, dst):
        copy = pltpu.make_async_copy(src, dst, load_sem.at[len(loads)])
        copy.start()
        loads.append(copy)

    for k in range(n_dp):
        load(grads_ref.at[:, pl.ds(k * cols, cols)], rep.at[k, me])
    for k in range(n_dp):
        load(q_ref.at[:, pl.ds(k * cols, cols)], qv.at[k])
    for j in range(experts):
        load(hidden_ref.at[j], hid.at[j])

    barrier = pltpu.get_barrier_semaphore()
    greeted = [along(k) for k in range(1, n_dp)] + [beside(i) for i in range(1, n_expert)]
    for peer in greeted:
        pl.semaphore_signal(barrier, inc=1, device_id=peer, device_id_type=MESH)
    routes[0, me] = jnp.concatenate([ids_ref[...].astype(F32), probs_ref[...]], axis=0)
    own_route = routes.at[0, me]
    pl.semaphore_wait(barrier, len(greeted))

    sent = []

    def push(src, dst, send_sem, recv_sem, device):
        copy = pltpu.make_async_remote_copy(
            src_ref=src, dst_ref=dst, send_sem=send_sem, recv_sem=recv_sem,
            device_id=device, device_id_type=MESH,
        )
        copy.start()
        sent.append(copy)
        return copy

    told, told_far, arrive_z = {}, {}, {}
    for i in range(1, n_expert):
        told[0, i] = push(
            own_route, own_route, route_send.at[0, i], route_recv.at[0, i], beside(i)
        )
    for k in range(1, n_dp):
        told_far[k] = push(own_route, routes.at[k, me], far_send.at[k], far_recv.at[k], along(k))

    arrive_one, arrive_two, arrive_core = {}, {}, {}

    def rows(b, k, h):
        own = rep.at[k, b] if k < n_dp else bulk.at[k - n_dp, b]
        return own.at[pl.ds(h * half, half)]

    def swap(k, h, first, second):
        part = rows(source(h, first, second, core), k, h)
        at = (h, k, first, second)
        partner = {"expert": block(spot[0], spot[1], 1 - core)}
        arrive_core[at] = push(part, part, core_send.at[at], core_recv.at[at], partner)

    def onward(k, h, first):
        part = rows(source(h, first, 0, core), k, h)
        for by in range(1, sides[1 - h]):
            at = (h, k, first, by - 1)
            arrive_two[at] = push(
                part, part, two_send.at[at], two_recv.at[at], {"expert": neighbour(1 - h, by)}
            )
        swap(k, h, first, 0)

    def begin(k):
        for h in range(2):
            part = rows(me, k, h)
            for by in range(1, sides[h]):
                at = (h, k, by - 1)
                arrive_one[at] = push(
                    part, part, one_send.at[at], one_recv.at[at], {"expert": neighbour(h, by)}
                )
        for h in range(2):
            onward(k, h, 0)

    def forward(k):
        for h in range(2):
            for by in range(1, sides[h]):
                arrive_one[h, k, by - 1].wait_recv()
                onward(k, h, by)

    def second(k, low=0, high=None):
        for h in range(2):
            for first in range(low, sides[h] if high is None else high):
                for by in range(1, sides[1 - h]):
                    arrive_two[h, k, first, by - 1].wait_recv()
                    swap(k, h, first, by)

    def landed(k):
        for at, copy in arrive_core.items():
            if at[1] == k:
                copy.wait_recv()

    def gain(k, p):
        piece = rep[k, pl.ds(p * span, span)].reshape(span * tokens, cols)
        value = lax.dot_general(
            qv[k], piece, (((1,), (1,)), ((), ())), preferred_element_type=F32
        )
        mixed[p] = value if k == 0 else mixed[p] + value

    def accumulate(k):
        loads[n_dp + k].wait()
        landed(k)
        for p in range(group):
            gain(k, p)

    def finish(k, far):
        for x in range(sides[0]):
            for y in range(sides[1]):
                if (x > 0 and y > 0) == far:
                    arrive_core[0, k, x, y].wait_recv()
                    arrive_core[1, k, y, x].wait_recv()
                    gain(k, source(0, x, y, 0) // 2)

    def place_tokens(k):
        for i in range(1, n_expert):
            told[k, i].wait_recv()
        ours = lax.broadcasted_iota(jnp.int32, (experts, tokens), 0) + me * experts
        ours = ours.astype(F32)
        gates, hits = [], []
        for b in range(n_expert):
            table = routes[k, b]
            value = jnp.zeros((experts, tokens), F32)
            hit = jnp.zeros((experts, tokens), F32)
            for t in range(top):
                same = table[t : t + 1, :] == ours
                value = jnp.where(same, table[top + t : top + t + 1, :], value)
                hit = jnp.where(same, 1.0, hit)
            gates.append(value)
            hits.append(hit)
        gate[k] = jnp.concatenate(gates, axis=1)
        hits = jnp.concatenate(hits, axis=0)
        before = lax.broadcasted_iota(jnp.int32, (tokens, tokens), 0)
        after = lax.broadcasted_iota(jnp.int32, (tokens, tokens), 1)
        earlier = jnp.where(before < after, 1.0, 0.0).astype(BF16)
        count = jnp.dot(hits.astype(BF16), earlier, preferred_element_type=F32)
        count = jnp.where(hits > 0.5, count, -float(slots))
        keys = [
            count[b * experts : (b + 1) * experts] + float(b * cap) for b in range(n_expert)
        ]
        key = jnp.concatenate(keys, axis=1).astype(jnp.int32)
        level = lax.broadcasted_iota(jnp.int32, (slots, n_expert * tokens), 0)
        for j in range(experts):
            pick[k, j] = jnp.where(level == key[j : j + 1, :], 1.0, 0.0).astype(BF16)

    for k in range(n_dp):
        loads[k].wait()
    for k in range(1, n_dp):
        to = lax.rem(z + k, n_dp)
        arrive_z[k] = push(
            rep.at[to, me], bulk.at[k - 1, me], z_send.at[k], z_recv.at[k], along(k)
        )
    for k in range(n_dp + 2):
        if k < n_dp:
            begin(k)
        if 0 <= k - 1 < n_dp:
            forward(k - 1)
        if k == 0:
            place_tokens(0)
        if k == n_dp:
            for r in range(1, n_dp):
                told_far[r].wait_recv()
                for i in range(1, n_expert):
                    told[r, i] = push(
                        routes.at[r, me], routes.at[r, me],
                        route_send.at[r, i], route_recv.at[r, i], beside(i),
                    )
            for r in range(1, n_dp):
                arrive_z[r].wait_recv()
                begin(n_dp + r - 1)
        if 0 <= k - 3 < n_dp - 1:
            accumulate(k - 3)
        if 0 <= k - 2 < n_dp - 1:
            second(k - 2)
        if k == n_dp + 1:
            second(n_dp - 1, 0, 1)
    loads[2 * n_dp - 1].wait()
    finish(n_dp - 1, False)
    second(n_dp - 1, 1)
    finish(n_dp - 1, True)
    for copy in loads[2 * n_dp :]:
        copy.wait()

    mate = z + 1 - 2 * lax.rem(z, 2)
    cross = n_dp - 1 - z
    inner = jnp.logical_or(z == 1, z == 2)

    def hop(kind, j, src, dst, to):
        return pltpu.make_async_remote_copy(
            src_ref=src.at[j], dst_ref=dst.at[j],
            send_sem=ring_send.at[kind, j], recv_sem=ring_recv.at[kind, j],
            device_id={"dp": to}, device_id_type=MESH,
        )

    def up(j):
        return hop(0, j, fact, got_up, mate)

    def over(j):
        return hop(1, j, fact, got_cross, cross)

    def down(j):
        return hop(2, j, tot, tot, mate)

    for j in range(experts):
        value = jnp.concatenate([mixed[p, j * rank : (j + 1) * rank] for p in range(group)], axis=1)
        value = (value * gate[0, j : j + 1, :]).astype(BF16)
        value = lax.dot_general(
            value, pick[0, j], (((1,), (1,)), ((), ())), preferred_element_type=F32
        ).astype(BF16)
        value = jnp.dot(value, hid[j], preferred_element_type=F32).astype(BF16)
        fact[2 * j : 2 * j + 2] = value.reshape(2, rank // 2, units)

        @pl.when(jnp.logical_not(inner))
        def _():
            up(2 * j).start()
            up(2 * j + 1).start()

    ahead = 3
    pieces = 2 * experts
    others = list(range(1, n_dp))
    for step in range(pieces + ahead):
        if step < pieces:

            @pl.when(inner)
            def _():
                up(step).wait_recv()
                fact[step] = (fact[step].astype(F32) + got_up[step].astype(F32)).astype(BF16)
                over(step).start()

        if step >= ahead:
            j = step - ahead

            @pl.when(inner)
            def _():
                over(j).wait_recv()
                tot[j] = (fact[j].astype(F32) + got_cross[j].astype(F32)).astype(BF16)
                down(j).start()

        if step % 2 == 1 and step // 2 < len(others):
            place_tokens(others[step // 2])
    for r in range(1, n_dp):
        forward(n_dp + r - 1)

    shape = (rank, 2 * rank)
    eye = lax.broadcasted_iota(jnp.int32, shape, 1) == lax.broadcasted_iota(jnp.int32, shape, 0) + rank
    eye = jnp.where(eye, 1.0, 0.0)
    for j in range(experts):

        @pl.when(jnp.logical_not(inner))
        def _():
            down(2 * j).wait_recv()
            down(2 * j + 1).wait_recv()

        one = tot[2 * j : 2 * j + 2].reshape(rank, units)
        doubled = jnp.concatenate([one, jnp.zeros_like(one)], axis=0)
        gram[j] = eye + lax.dot_general(
            one, doubled, (((1,), (1,)), ((), ())), preferred_element_type=F32
        )

    table = [gram[:, k, :].T for k in range(rank)]
    for k in range(rank):
        row = table[k]
        scaled = row * (1.0 / row[k : k + 1, :])
        for i in range(k + 1, rank):
            table[i] = table[i] - row[i : i + 1, :] * scaled
        table[k] = row * lax.rsqrt(row[k : k + 1, :])
    for k in range(rank):
        gram[:, k, :] = table[k].T

    batch = experts // 2
    arrive_proj, stored = {}, []

    def put(src, dst):
        copy = pltpu.make_async_copy(src, dst, out_sem.at[len(stored)])
        copy.start()
        stored.append(copy)

    for j in range(experts):
        inverse = gram[j][:, rank:]
        high = inverse.astype(BF16)
        low = (inverse - high.astype(F32)).astype(BF16)
        one = tot[2 * j : 2 * j + 2].reshape(rank, units)
        value = jnp.dot(high, one, preferred_element_type=F32)
        value = value + jnp.dot(low, one, preferred_element_type=F32)
        basis[j] = value * math.sqrt(units)
        value = value.astype(BF16)
        proj[0, j // 2, :, (j % 2) * slots : (j % 2 + 1) * slots] = lax.dot_general(
            value, hid[j], (((1,), (1,)), ((), ())), preferred_element_type=F32
        ).astype(BF16)
        if (j + 1) % batch == 0:
            g = j // batch
            put(basis.at[pl.ds(g * batch, batch)], basis_ref.at[pl.ds(g * batch, batch)])
            part = pl.ds(g * batch // 2, batch // 2)
            for k in range(1, n_dp):
                arrive_proj[k, g] = push(
                    proj.at[0, part], proj.at[k, part],
                    proj_send.at[k, g], proj_recv.at[k, g], along(k),
                )

    def update(k):
        if k:
            for g in range(2):
                arrive_proj[k, g].wait_recv()
        for j in range(experts):
            value = jnp.dot(
                proj[k, j // 2, :, (j % 2) * slots : (j % 2 + 1) * slots], pick[k, j],
                preferred_element_type=F32,
            )
            spr[j * rank : (j + 1) * rank] = (value * gate[k, j : j + 1, :]).astype(BF16)
        if k:
            landed(n_dp + k - 1)
        own = bulk.at[k - 1] if k else rep.at[z]

        width = 256 if cols % 256 == 0 else 128
        for c in range(cols // width):
            at = slice(c * width, (c + 1) * width)
            right = own[:, :, at].reshape(n_expert * tokens, width)
            value = jnp.dot(spr[...], right, preferred_element_type=F32)
            upd[:, at] = upd[:, at] + value if k else value
            if k == n_dp - 1:
                put(upd.at[:, at], upd_ref.at[:, at])

    update(0)
    for r in range(1, n_dp):
        second(n_dp + r - 1)
    for r in range(1, n_dp):
        update(r)
    for j in range(pieces):

        @pl.when(inner)
        def _():
            over(j).wait_send()
            down(j).wait_send()

        @pl.when(jnp.logical_not(inner))
        def _():
            up(j).wait_send()

    for copy in sent:
        copy.wait_send()
    for copy in stored:
        copy.wait()


def fused_buffers(n_expert, n_dp, tokens, width, experts, slots, units, rank, top):
    cols = width // n_dp
    return [
        ((n_dp, n_expert, tokens, cols), BF16),
        ((n_dp - 1, n_expert, tokens, cols), BF16),
        ((experts, slots, units), BF16),
        ((n_dp, experts * rank, cols), BF16),
        ((n_dp, n_expert, 2 * top, tokens), F32),
        ((n_dp, experts, n_expert * tokens), F32),
        ((n_dp, experts, slots, n_expert * tokens), BF16),
        ((n_expert // 2, experts * rank, 2 * tokens), F32),
        ((2 * experts, rank // 2, units), BF16),
        ((2 * experts, rank // 2, units), BF16),
        ((2 * experts, rank // 2, units), BF16),
        ((2 * experts, rank // 2, units), BF16),
        ((experts, rank, 2 * rank), F32),
        ((n_dp, experts // 2, rank, 2 * slots), BF16),
        ((experts * rank, n_expert * tokens), BF16),
        ((experts, rank, units), F32),
        ((experts * rank, cols), F32),
    ]


def fused(grads, ids, probs, hidden, q, buffers):
    n_expert, n_dp = lax.axis_size("expert"), lax.axis_size("dp")
    experts, slots, units = hidden.shape
    rank = q.shape[0] // experts
    cols = q.shape[1] // n_dp
    chips = n_expert // 2
    long = max(math.isqrt(chips), chips // math.isqrt(chips))
    tags = 2 * n_dp - 1
    dma = pltpu.SemaphoreType.DMA
    vmem = pl.BlockSpec(memory_space=pltpu.VMEM)
    anywhere = pl.BlockSpec(memory_space=pl.ANY)
    return pl.pallas_call(
        functools.partial(fused_kernel, n_expert, n_dp),
        out_shape=(
            jax.ShapeDtypeStruct((experts, rank, units), F32),
            jax.ShapeDtypeStruct((experts * rank, cols), F32),
        ),
        in_specs=[anywhere, vmem, vmem, anywhere, anywhere],
        out_specs=(anywhere, anywhere),
        scratch_shapes=[pltpu.VMEM(*b) for b in buffers] + [
            dma((2 + cols // 128,)), dma((2 * n_dp + experts,)),
            dma((n_dp, n_expert)), dma((n_dp, n_expert)), dma((n_dp,)), dma((n_dp,)),
            dma((n_dp,)), dma((n_dp,)),
            dma((2, tags, long - 1)), dma((2, tags, long - 1)),
            dma((2, tags, long, long - 1)), dma((2, tags, long, long - 1)),
            dma((2, tags, long, long)), dma((2, tags, long, long)),
            dma((3, 2 * experts)), dma((3, 2 * experts)), dma((n_dp, 2)), dma((n_dp, 2)),
        ],
        compiler_params=pltpu.CompilerParams(
            collective_id=2, has_side_effects=True, vmem_limit_bytes=67043328
        ),
        name="fused",
    )(grads, ids, probs, hidden, q)


def local(out_grads, expert_ids, gate_probs, hidden_acts, q_previous):
    n_expert, n_dp = lax.axis_size("expert"), lax.axis_size("dp")
    experts, slots, units = hidden_acts.shape[1:]
    tokens, width = out_grads.shape[1:]
    rank = q_previous.shape[1]
    cols = width // n_dp
    buffers = fused_buffers(
        n_expert, n_dp, tokens, width, experts, slots, units, rank, expert_ids.shape[2]
    )
    held = sum(math.prod(shape) * jnp.dtype(kind).itemsize for shape, kind in buffers)
    if n_dp != 4 or held > 60 * 2**20:
        return spacious(out_grads, expert_ids, gate_probs, hidden_acts, q_previous)
    q = q_previous.reshape(experts * rank, width)
    basis, update = fused(out_grads[0], expert_ids[0].T, gate_probs[0].T, hidden_acts[0], q, buffers)
    return (basis, update.reshape(experts, rank, cols))


def spacious(out_grads, expert_ids, gate_probs, hidden_acts, q_previous):
    n_expert = lax.axis_size("expert")
    n_dp = lax.axis_size("dp")
    experts, slots, units = hidden_acts.shape[1:]
    capacity = slots // n_expert
    tokens, width = out_grads.shape[1:]
    top = expert_ids.shape[2]
    rank = q_previous.shape[1]
    cols = width // n_dp
    first = lax.axis_index("expert") * experts

    route = jnp.concatenate([expert_ids[0].astype(F32), gate_probs[0]], axis=1).T
    grads, route = gathered(out_grads[0], route)
    mine = (first + jnp.arange(experts)).astype(F32)[:, None]
    ids = route[:, :, :top].transpose(2, 0, 1, 3)[:, :, :, None, :]
    weight = route[:, :, top:].transpose(2, 0, 1, 3)[:, :, :, None, :]
    hit = ids == mine
    gate = jnp.sum(jnp.where(hit, weight, 0.0), axis=0)
    chosen = jnp.any(hit, axis=0)
    earlier = (jnp.arange(tokens)[:, None] < jnp.arange(tokens)[None, :]).astype(BF16)
    place = jnp.einsum("pbjt,tu->pbju", chosen.astype(BF16), earlier, preferred_element_type=F32)
    place = jnp.where(chosen, place, -1.0)
    pick = (place[:, :, :, None, :] == jnp.arange(capacity, dtype=F32)[:, None]).astype(BF16)

    q_part = lax.dynamic_slice_in_dim(q_previous, lax.axis_index("dp") * cols, cols, 2)
    mixed = jnp.einsum("jrd,bptd->jrbpt", q_part, grads, preferred_element_type=F32)
    scale = gate.transpose(2, 1, 0, 3)
    mixed = (mixed * scale[:, None]).astype(BF16)
    part = jnp.einsum("jrbpt,pbjct->pjrbc", mixed, pick, preferred_element_type=F32).astype(BF16)
    part = part.reshape(n_dp, experts, rank, slots)
    ortho, proj = factors(part, hidden_acts[0], n_dp)
    proj = proj.reshape(n_dp, experts, rank, n_expert, capacity)
    spread = jnp.einsum("pjrbc,pbjct->jrbpt", proj, pick, preferred_element_type=F32)
    spread = (spread * scale[:, None]).astype(BF16)
    q_update = jnp.einsum("jrbpt,bptd->jrd", spread, grads, preferred_element_type=F32)
    new_basis = ortho.astype(F32) * math.sqrt(units)
    return (new_basis, q_update)


def solution(mesh):
    return jax.shard_map(
        local,
        mesh=mesh,
        in_specs=(
            P("dp", "expert", None),
            P("dp", "expert", None),
            P("dp", "expert", None),
            P("dp", "expert", None, None),
            P("expert", None, None),
        ),
        out_specs=(P("expert", None, None), P("expert", None, "dp")),
        check_vma=False,
    )
```

```python
import functools
import math

import jax
import jax.numpy as jnp
from jax import lax
from jax.experimental import pallas as pl
from jax.experimental.pallas import tpu as pltpu
from jax.sharding import PartitionSpec as P

F32, BF16 = jnp.float32, jnp.bfloat16


MESH = pl.DeviceIdType.MESH


def orthonormal(value):
    rank = value[0].shape[0]
    rows = lax.broadcasted_iota(jnp.int32, (rank, 2 * rank), 0)
    cols = lax.broadcasted_iota(jnp.int32, (rank, 2 * rank), 1)
    eye = (cols == rows + rank).astype(F32)
    tables = []
    for one in value:
        doubled = jnp.concatenate([one, jnp.zeros_like(one)], axis=0)
        gram = lax.dot_general(
            one, doubled, (((1,), (1,)), ((), ())),
            precision=lax.Precision.HIGHEST, preferred_element_type=F32,
        )
        tables.append(gram + eye)
    for k in range(rank):
        for j, table in enumerate(tables):
            row = table[k : k + 1, :]
            pivot = lax.rsqrt(row[:, k : k + 1])
            scaled = row * pivot
            column = table[:, k : k + 1] * pivot
            table = jnp.where(rows > k, table - column * scaled, table)
            tables[j] = jnp.where(rows == k, scaled, table)
    return [
        jnp.dot(
            table[:, rank:], one, precision=lax.Precision.HIGHEST, preferred_element_type=F32
        )
        for table, one in zip(tables, value)
    ]


def factor_kernel(
    n, part_ref, hidden_ref, ortho_ref, proj_ref,
    hidden, got_part, fact, got_fact, load_sem, send_sem, recv_sem,
):
    me = lax.axis_index("dp")
    experts = hidden.shape[0]
    per = experts // n
    peers = [lax.rem(me + offset, n) for offset in range(1, n)]
    loads = []
    for j in range(experts):
        load = pltpu.make_async_copy(hidden_ref.at[j], hidden.at[j], load_sem.at[j])
        load.start()
        loads.append(load)
    barrier = pltpu.get_barrier_semaphore()
    for peer in peers:
        pl.semaphore_signal(barrier, inc=1, device_id={"dp": peer}, device_id_type=MESH)
    pl.semaphore_wait(barrier, n - 1)

    def push(phase, offset, source, target):
        copy = pltpu.make_async_remote_copy(
            src_ref=source,
            dst_ref=target,
            send_sem=send_sem.at[phase, offset],
            recv_sem=recv_sem.at[phase, offset],
            device_id={"dp": peers[offset]},
            device_id_type=MESH,
        )
        copy.start()
        return copy

    sent = [push(0, o, part_ref.at[peers[o]], got_part.at[o]) for o in range(n - 1)]
    for copy in sent:
        copy.wait()
    mixed = part_ref[me].astype(F32)
    for o in range(n - 1):
        mixed = mixed + got_part[o].astype(F32)
    mixed = mixed.astype(BF16)
    for load in loads:
        load.wait()
    rank = mixed.shape[1]
    for j in range(experts):
        fact[j] = jnp.dot(mixed[j], hidden[j], preferred_element_type=F32).astype(BF16)
    sent = [
        push(1, o, fact.at[pl.ds(peers[o] * per, per)], got_fact.at[o]) for o in range(n - 1)
    ]
    for copy in sent:
        copy.wait()
    share = []
    for i in range(per):
        total = fact[me * per + i].astype(F32)
        for o in range(n - 1):
            total = total + got_fact[o, i].astype(F32)
        share.append(total)
    for i, value in enumerate(orthonormal(share)):
        ortho_ref[me * per + i] = value.astype(BF16)
    mine = ortho_ref.at[pl.ds(me * per, per)]
    sent = [push(2, o, mine, mine) for o in range(n - 1)]

    def project(group):
        for i in range(per):
            j = group * per + i
            proj_ref[me, j] = lax.dot_general(
                ortho_ref[j], hidden[j], (((1,), (1,)), ((), ())), preferred_element_type=F32
            ).astype(BF16)

    project(me)
    for o in range(n - 1):
        sent[o].wait()
        project(lax.rem(me + n - 1 - o, n))
    sent = [push(3, o, proj_ref.at[me], proj_ref.at[me]) for o in range(n - 1)]
    for copy in sent:
        copy.wait()


def factors(part, hidden, n):
    experts, slots, units = hidden.shape
    rank = part.shape[2]
    per = experts // n
    vmem = pl.BlockSpec(memory_space=pltpu.VMEM)
    return pl.pallas_call(
        functools.partial(factor_kernel, n),
        out_shape=(
            jax.ShapeDtypeStruct((experts, rank, units), BF16),
            jax.ShapeDtypeStruct((n, experts, rank, slots), BF16),
        ),
        in_specs=[vmem, pl.BlockSpec(memory_space=pl.ANY)],
        out_specs=(vmem, vmem),
        scratch_shapes=[
            pltpu.VMEM((experts, slots, units), BF16),
            pltpu.VMEM((n - 1, experts, rank, slots), BF16),
            pltpu.VMEM((experts, rank, units), BF16),
            pltpu.VMEM((n - 1, per, rank, units), BF16),
            pltpu.SemaphoreType.DMA((experts,)),
            pltpu.SemaphoreType.DMA((4, n - 1)),
            pltpu.SemaphoreType.DMA((4, n - 1)),
        ],
        compiler_params=pltpu.CompilerParams(
            collective_id=0, has_side_effects=True, vmem_limit_bytes=40 * 2**20
        ),
        name="factors",
    )(part, hidden)


def gather_kernel(
    n_expert, n_dp, x_ref, route_ref, all_ref, routes_ref,
    route_send, route_recv, own_sem, z_send, z_recv, one_send, one_recv, two_send, two_recv, core_send, core_recv,
):
    me, z = lax.axis_index("expert"), lax.axis_index("dp")
    chips = n_expert // 2
    wide = math.isqrt(chips)
    sides = (wide, chips // wide)
    core, chip = lax.rem(me, 2), me // 2
    spot = (lax.rem(chip, wide), chip // wide)
    half, cols = x_ref.shape[0] // 2, all_ref.shape[3]

    def shifted(dim, by):
        return lax.rem(spot[dim] + by + sides[dim], sides[dim])

    def block(x, y, c):
        return (y * wide + x) * 2 + c

    def neighbour(dim, by):
        moved = shifted(dim, by)
        return block(moved, spot[1], core) if dim == 0 else block(spot[0], moved, core)

    def source(dim, first, second, c):
        x, y = (first, second) if dim == 0 else (second, first)
        return block(shifted(0, -x), shifted(1, -y), c)

    barrier = pltpu.get_barrier_semaphore()
    def greet(i, carry):
        pl.semaphore_signal(barrier, inc=1, device_id=other_of(i), device_id_type=MESH)
        return carry

    def other_of(i):
        return {
            "expert": lax.rem(me + lax.rem(i, n_expert), n_expert),
            "dp": lax.rem(z + i // n_expert, n_dp),
        }

    total = n_expert * n_dp
    lax.fori_loop(1, total, greet, 0)
    pl.semaphore_wait(barrier, total - 1)

    sent = []
    mine = routes_ref.at[z, me]
    routes_ref[z, me] = route_ref[...]

    def push(src, dst, send_sem, recv_sem, device):
        copy = pltpu.make_async_remote_copy(
            src_ref=src, dst_ref=dst, send_sem=send_sem, recv_sem=recv_sem,
            device_id=device, device_id_type=MESH,
        )
        copy.start()
        sent.append(copy)
        return copy

    def columns(r):
        return x_ref.at[:, pl.ds(pl.multiple_of(r * cols, 128), cols)]

    own = pltpu.make_async_copy(columns(z), all_ref.at[me, z], own_sem)
    own.start()
    arrive_z, arrive_one, arrive_two, arrive_core = {}, {}, {}, []
    for k in range(1, n_dp):
        to = lax.rem(z + k, n_dp)
        arrive_z[k] = push(
            columns(to), all_ref.at[me, z], z_send.at[k - 1], z_recv.at[k - 1], {"dp": to}
        )

    def tell(i, carry):
        pltpu.make_async_remote_copy(
            src_ref=route_ref, dst_ref=mine, send_sem=route_send.at[i],
            recv_sem=route_recv.at[i], device_id=other_of(i), device_id_type=MESH,
        ).start()
        return carry

    lax.fori_loop(1, total, tell, 0)

    def rows(b, k, h):
        return all_ref.at[b, lax.rem(z - k + n_dp, n_dp), pl.ds(h * half, half)]

    def swap(k, h, first, second):
        part = rows(source(h, first, second, core), k, h)
        at = (h, k, first, second)
        partner = {"expert": block(spot[0], spot[1], 1 - core)}
        arrive_core.append(push(part, part, core_send.at[at], core_recv.at[at], partner))

    def onward(k, h, first):
        part = rows(source(h, first, 0, core), k, h)
        for by in range(1, sides[1 - h]):
            at = (h, k, first, by - 1)
            arrive_two[at] = push(
                part, part, two_send.at[at], two_recv.at[at], {"expert": neighbour(1 - h, by)}
            )
        swap(k, h, first, 0)

    for k in range(n_dp + 2):
        if k < n_dp:
            if k:
                arrive_z[k].wait_recv()
            else:
                own.wait()
            for h in range(2):
                part = rows(me, k, h)
                for by in range(1, sides[h]):
                    at = (h, k, by - 1)
                    arrive_one[at] = push(
                        part, part, one_send.at[at], one_recv.at[at], {"expert": neighbour(h, by)}
                    )
            for h in range(2):
                onward(k, h, 0)
        if 0 <= k - 1 < n_dp:
            for h in range(2):
                for by in range(1, sides[h]):
                    arrive_one[(h, k - 1, by - 1)].wait_recv()
                    onward(k - 1, h, by)
        if 0 <= k - 2 < n_dp:
            for h in range(2):
                for first in range(sides[h]):
                    for by in range(1, sides[1 - h]):
                        arrive_two[(h, k - 2, first, by - 1)].wait_recv()
                        swap(k - 2, h, first, by)
    def told(i, carry):
        pltpu.make_async_remote_copy(
            src_ref=route_ref, dst_ref=mine, send_sem=route_send.at[i],
            recv_sem=route_recv.at[i], device_id=other_of(i), device_id_type=MESH,
        ).wait()
        return carry

    lax.fori_loop(1, total, told, 0)
    for copy in arrive_core:
        copy.wait_recv()
    for copy in sent:
        copy.wait_send()


def gathered(grads, route):
    n_expert, n_dp = lax.axis_size("expert"), lax.axis_size("dp")
    tokens, width = grads.shape
    long = max(math.isqrt(n_expert // 2), n_expert // 2 // math.isqrt(n_expert // 2))
    dma = pltpu.SemaphoreType.DMA
    return pl.pallas_call(
        functools.partial(gather_kernel, n_expert, n_dp),
        out_shape=(
            jax.ShapeDtypeStruct((n_expert, n_dp, tokens, width // n_dp), grads.dtype),
            jax.ShapeDtypeStruct((n_dp, n_expert, *route.shape), route.dtype),
        ),
        in_specs=[pl.BlockSpec(memory_space=pltpu.VMEM)] * 2,
        out_specs=(pl.BlockSpec(memory_space=pl.ANY), pl.BlockSpec(memory_space=pltpu.VMEM)),
        scratch_shapes=[
            dma((n_expert * n_dp,)), dma((n_expert * n_dp,)), dma(()), dma((n_dp - 1,)), dma((n_dp - 1,)),
            dma((2, n_dp, long)), dma((2, n_dp, long)),
            dma((2, n_dp, long, long)), dma((2, n_dp, long, long)),
            dma((2, n_dp, long, long)), dma((2, n_dp, long, long)),
        ],
        compiler_params=pltpu.CompilerParams(
            collective_id=1, has_side_effects=True, vmem_limit_bytes=56 * 2**20
        ),
        name="gather_rows",
    )(grads, route)


def fused_kernel(
    n_expert, n_dp, grads_ref, ids_ref, probs_ref, hidden_ref, q_ref, basis_ref, upd_ref,
    rep, own, hid, qall, routes, gate, pick, near_gate, near_pick, weighed, message, parts, spots,
    fact, got_up, got_cross, tot, gram, proj, spr,
    basis, upd, plane_sem, out_sem, load_sem, route_send, route_recv, far_send, far_recv, z_send, z_recv,
    one_send, one_recv, two_send, two_recv, core_send, core_recv, part_send, part_recv,
    ring_send, ring_recv, proj_send, proj_recv,
):
    me, z = lax.axis_index("expert"), lax.axis_index("dp")
    chips = n_expert // 2
    wide = math.isqrt(chips)
    sides = (wide, chips // wide)
    core, chip = lax.rem(me, 2), me // 2
    spot = (lax.rem(chip, wide), chip // wide)
    tokens, cols = rep.shape[2:]
    experts, slots, units = hid.shape
    rank = 2 * fact.shape[1]
    cap = slots // n_expert
    top = routes.shape[2] // 2
    mate = z + 1 - 2 * lax.rem(z, 2)
    cross = n_dp - 1 - z
    replica = [z, cross, mate, lax.rem(z + 2, n_dp)]
    order = [0, 2, 1, 3]

    def shifted(dim, by):
        return lax.rem(spot[dim] + by + sides[dim], sides[dim])

    def block(x, y, c):
        return (y * wide + x) * 2 + c

    def neighbour(dim, by):
        moved = shifted(dim, by)
        return block(moved, spot[1], core) if dim == 0 else block(spot[0], moved, core)

    def source(dim, first, second, c):
        x, y = (first, second) if dim == 0 else (second, first)
        return block(shifted(0, -x), shifted(1, -y), c)

    def beside(i):
        return {"expert": lax.rem(me + i, n_expert)}

    def quarter(ref, at):
        return ref.at[:, pl.ds(pl.multiple_of(at * cols, 128), cols)]

    loads = []

    def load(src, dst):
        copy = pltpu.make_async_copy(src, dst, load_sem.at[len(loads)])
        copy.start()
        loads.append(copy)

    for m in (1, 3, 2):
        load(quarter(grads_ref, replica[m]), own.at[m - 1])
    load(quarter(q_ref, z), qall.at[me])
    load(quarter(grads_ref, z), rep.at[0, me])
    for j in range(experts):
        load(hidden_ref.at[j], hid.at[j])

    barrier = pltpu.get_barrier_semaphore()
    greeted = [{"dp": replica[m]} for m in range(1, n_dp)]
    greeted += [beside(i) for i in range(1, n_expert)]
    for peer in greeted:
        pl.semaphore_signal(barrier, inc=1, device_id=peer, device_id_type=MESH)
    routes[0, me] = jnp.concatenate([ids_ref[...].astype(F32), probs_ref[...]], axis=0)
    own_route = routes.at[0, me]
    pl.semaphore_wait(barrier, len(greeted))
    for m in range(1, n_dp):
        pl.semaphore_signal(
            plane_sem, inc=1, device_id={"dp": replica[m]}, device_id_type=MESH
        )

    sent = []

    def push(src, dst, send_sem, recv_sem, device):
        copy = pltpu.make_async_remote_copy(
            src_ref=src, dst_ref=dst, send_sem=send_sem, recv_sem=recv_sem,
            device_id=device, device_id_type=MESH,
        )
        copy.start()
        sent.append(copy)
        return copy

    told, told_far, arrive_z = {}, {}, {}
    for m in (1, 3, 2):
        told_far[m] = push(
            own_route, routes.at[m, me], far_send.at[m], far_recv.at[m], {"dp": replica[m]}
        )
    for at, m in enumerate((1, 3, 2)):
        loads[at].wait()
        arrive_z[m] = push(
            own.at[m - 1], rep.at[m, me], z_send.at[m], z_recv.at[m], {"dp": replica[m]}
        )

    arrive_one, arrive_two, arrive_core = {}, {}, {}

    def rows(b, k, h):
        whole = rep.at[k, b] if k < n_dp else qall.at[b]
        half = whole.shape[0] // 2
        return whole.at[pl.ds(h * half, half)]

    def swap(k, h, first, second):
        part = rows(source(h, first, second, core), k, h)
        at = (h, k, first, second)
        partner = {"expert": block(spot[0], spot[1], 1 - core)}
        arrive_core[at] = push(part, part, core_send.at[at], core_recv.at[at], partner)

    def onward(k, h, first):
        part = rows(source(h, first, 0, core), k, h)
        for by in range(1, sides[1 - h]):
            at = (h, k, first, by - 1)
            arrive_two[at] = push(
                part, part, two_send.at[at], two_recv.at[at], {"expert": neighbour(1 - h, by)}
            )
        swap(k, h, first, 0)

    def begin(k):
        for h in range(2):
            part = rows(me, k, h)
            for by in range(1, sides[h]):
                at = (h, k, by - 1)
                arrive_one[at] = push(
                    part, part, one_send.at[at], one_recv.at[at], {"expert": neighbour(h, by)}
                )
        for h in range(2):
            onward(k, h, 0)

    def forward(k):
        for h in range(2):
            for by in range(1, sides[h]):
                arrive_one[h, k, by - 1].wait_recv()
                onward(k, h, by)

    def second(k):
        for h in range(2):
            for first in range(sides[h]):
                for by in range(1, sides[1 - h]):
                    arrive_two[h, k, first, by - 1].wait_recv()
                    swap(k, h, first, by)

    def landed(k):
        for at, copy in arrive_core.items():
            if at[1] == k:
                copy.wait_recv()

    def matched(table, first, count):
        ours = lax.broadcasted_iota(jnp.int32, (count, tokens), 0) + first
        ours = ours.astype(F32)
        value = jnp.zeros((count, tokens), F32)
        hit = jnp.zeros((count, tokens), F32)
        for t in range(top):
            same = table[t : t + 1, :] == ours
            value = jnp.where(same, table[top + t : top + t + 1, :], value)
            hit = jnp.where(same, 1.0, hit)
        return value, hit

    def positions(hits):
        before = lax.broadcasted_iota(jnp.int32, (tokens, tokens), 0)
        after = lax.broadcasted_iota(jnp.int32, (tokens, tokens), 1)
        earlier = jnp.where(before < after, 1.0, 0.0).astype(BF16)
        count = jnp.dot(hits.astype(BF16), earlier, preferred_element_type=F32)
        return jnp.where(hits > 0.5, count, -float(slots))

    def place_tokens(k):
        for i in range(1, n_expert):
            told[k, i].wait_recv()
        found = [matched(routes[k, b], me * experts, experts) for b in range(n_expert)]
        gate[k] = jnp.concatenate([value for value, _ in found], axis=1)
        count = positions(jnp.concatenate([hit for _, hit in found], axis=0))
        keys = [
            count[b * experts : (b + 1) * experts] + float(b * cap) for b in range(n_expert)
        ]
        key = jnp.concatenate(keys, axis=1).astype(jnp.int32)
        level = lax.broadcasted_iota(jnp.int32, (slots, n_expert * tokens), 0)
        for j in range(experts):
            pick[k, j] = jnp.where(level == key[j : j + 1, :], 1.0, 0.0).astype(BF16)

    def place_near(m):
        value, hit = matched(routes[m, me], 0, n_expert * experts)
        near_gate[m] = value
        key = positions(hit).astype(jnp.int32)
        level = lax.broadcasted_iota(jnp.int32, (cap, tokens), 0)
        for b in range(n_expert):
            rows_of = [
                jnp.where(level == key[b * experts + j : b * experts + j + 1, :], 1.0, 0.0)
                for j in range(experts)
            ]
            near_pick[m, b] = jnp.concatenate(rows_of, axis=0).astype(BF16)

    def folded(value, count, size):
        line = lax.broadcasted_iota(jnp.int32, (rank, value.shape[1]), 1)
        out = jnp.zeros((rank, value.shape[1]), F32)
        for j in range(count):
            mine = jnp.logical_and(line >= j * size, line < (j + 1) * size)
            out = jnp.where(mine, value[j * rank : (j + 1) * rank], out)
        return out

    arrive_part = {}

    def contract(ms):
        for i in range(n_expert):
            b = lax.rem(me + i, n_expert)
            near = jnp.concatenate([rep[m, me] for m in ms], axis=0)
            value = lax.dot_general(
                qall[b], near, (((1,), (1,)), ((), ())), preferred_element_type=F32
            )
            for at, m in enumerate(ms):
                scale = near_gate[m, pl.ds(pl.multiple_of(b * experts, experts), experts)]
                one = value[:, at * tokens : (at + 1) * tokens]
                one = one.reshape(experts, rank, tokens) * scale[:, None, :]
                weighed[at, i] = one.reshape(experts * rank, tokens).astype(BF16)
        for at, m in enumerate(ms):
            for i in range(n_expert):
                b = lax.rem(me + i, n_expert)
                value = lax.dot_general(
                    weighed[at, i], near_pick[m, b], (((1,), (1,)), ((), ())),
                    preferred_element_type=F32,
                )
                message[m, i] = folded(value, experts, cap).astype(BF16)
        for m in ms:
            for i in range(n_expert):
                if m == 0 and i == 0:
                    parts[0, me] = message[0, 0]
                    continue
                arrive_part[m, i] = push(
                    message.at[m, i], parts.at[m, me], part_send.at[m, i], part_recv.at[m, i],
                    {"expert": lax.rem(me + i, n_expert), "dp": replica[m]},
                )

    loads[3].wait()
    begin(n_dp)
    across = lax.broadcasted_iota(jnp.int32, (slots, slots), 0)
    along = lax.broadcasted_iota(jnp.int32, (slots, slots), 1)
    along = along - cap * (along // cap)
    for j in range(experts):
        spots[j] = jnp.where(across == along + j * cap, 1.0, 0.0).astype(BF16)
    for copy in loads[4:]:
        copy.wait()
    place_near(0)
    forward(n_dp)
    begin(0)
    for m in range(1, n_dp):
        told_far[m].wait_recv()
        place_near(m)
    second(n_dp)
    pl.semaphore_wait(plane_sem, n_dp - 1)
    arrive_z[2].wait_recv()
    landed(n_dp)
    contract((0, 2))
    arrive_z[1].wait_recv()
    contract((1,))
    arrive_z[3].wait_recv()
    contract((3,))
    forward(0)
    for m in order:
        for i in range(1, n_expert):
            told[m, i] = push(
                routes.at[m, me], routes.at[m, me],
                route_send.at[m, i], route_recv.at[m, i], beside(i),
            )
    for m in order[1:]:
        begin(m)

    inner = jnp.logical_or(z == 1, z == 2)

    def hop(kind, j, src, dst, to):
        return pltpu.make_async_remote_copy(
            src_ref=src.at[j], dst_ref=dst.at[j],
            send_sem=ring_send.at[kind, j], recv_sem=ring_recv.at[kind, j],
            device_id={"dp": to}, device_id_type=MESH,
        )

    def up(j):
        return hop(0, j, fact, got_up, mate)

    def over(j):
        return hop(1, j, fact, got_cross, cross)

    def down(j):
        return hop(2, j, tot, tot, mate)

    for copy in arrive_part.values():
        copy.wait_recv()
    filled = []
    for b in range(n_expert):
        value = parts[0, b].astype(F32)
        for m in range(1, n_dp):
            value = value + parts[m, b].astype(F32)
        filled.append(value.astype(BF16))
    filled = jnp.concatenate(filled, axis=0)
    for j in range(experts):
        value = jnp.dot(filled, spots[j], preferred_element_type=F32)
        value = folded(value, n_expert, cap).astype(BF16)
        value = jnp.dot(value, hid[j], preferred_element_type=F32).astype(BF16)
        fact[2 * j : 2 * j + 2] = value.reshape(2, rank // 2, units)

        @pl.when(jnp.logical_not(inner))
        def _():
            up(2 * j).start()
            up(2 * j + 1).start()

    ahead = 3
    pieces = 2 * experts
    for step in range(pieces + ahead):
        if step < pieces:

            @pl.when(inner)
            def _():
                up(step).wait_recv()
                fact[step] = (fact[step].astype(F32) + got_up[step].astype(F32)).astype(BF16)
                over(step).start()

        if step >= ahead:
            j = step - ahead

            @pl.when(inner)
            def _():
                over(j).wait_recv()
                tot[j] = (fact[j].astype(F32) + got_cross[j].astype(F32)).astype(BF16)
                down(j).start()

        if step in (1, 3, 5, 7):
            place_tokens(order[step // 2])
        if step == 9:
            forward(2)
        if step == 13:
            forward(1)
        if step == 17:
            forward(3)

    shape = (rank, 2 * rank)
    eye = lax.broadcasted_iota(jnp.int32, shape, 1) == lax.broadcasted_iota(jnp.int32, shape, 0) + rank
    eye = jnp.where(eye, 1.0, 0.0)
    for j in range(experts):

        @pl.when(jnp.logical_not(inner))
        def _():
            down(2 * j).wait_recv()
            down(2 * j + 1).wait_recv()

        one = tot[2 * j : 2 * j + 2].reshape(rank, units)
        doubled = jnp.concatenate([one, jnp.zeros_like(one)], axis=0)
        gram[j] = eye + lax.dot_general(
            one, doubled, (((1,), (1,)), ((), ())), preferred_element_type=F32
        )

    table = [gram[:, k, :].T for k in range(rank)]
    for k in range(rank):
        row = table[k]
        scaled = row * (1.0 / row[k : k + 1, :])
        for i in range(k + 1, rank):
            table[i] = table[i] - row[i : i + 1, :] * scaled
        table[k] = row * lax.rsqrt(row[k : k + 1, :])
    for k in range(rank):
        gram[:, k, :] = table[k].T

    batch = experts // 2
    arrive_proj, stored = {}, []

    def put(src, dst):
        copy = pltpu.make_async_copy(src, dst, out_sem.at[len(stored)])
        copy.start()
        stored.append(copy)

    for j in range(experts):
        inverse = gram[j][:, rank:]
        high = inverse.astype(BF16)
        low = (inverse - high.astype(F32)).astype(BF16)
        one = tot[2 * j : 2 * j + 2].reshape(rank, units)
        value = jnp.dot(high, one, preferred_element_type=F32)
        value = value + jnp.dot(low, one, preferred_element_type=F32)
        basis[j] = value * math.sqrt(units)
        value = value.astype(BF16)
        proj[0, j // 2, :, (j % 2) * slots : (j % 2 + 1) * slots] = lax.dot_general(
            value, hid[j], (((1,), (1,)), ((), ())), preferred_element_type=F32
        ).astype(BF16)
        if (j + 1) % batch == 0:
            g = j // batch
            put(basis.at[pl.ds(g * batch, batch)], basis_ref.at[pl.ds(g * batch, batch)])
            part = pl.ds(g * batch // 2, batch // 2)
            for k in (3, 1, 2):
                arrive_proj[k, g] = push(
                    proj.at[0, part], proj.at[k, part],
                    proj_send.at[k, g], proj_recv.at[k, g], {"dp": replica[k]},
                )

    def update(k):
        if k:
            for g in range(2):
                arrive_proj[k, g].wait_recv()
        for j in range(experts):
            value = jnp.dot(
                proj[k, j // 2, :, (j % 2) * slots : (j % 2 + 1) * slots], pick[k, j],
                preferred_element_type=F32,
            )
            spr[j * rank : (j + 1) * rank] = (value * gate[k, j : j + 1, :]).astype(BF16)
        landed(k)
        width = 256 if cols % 256 == 0 else 128
        for c in range(cols // width):
            at = slice(c * width, (c + 1) * width)
            right = rep[k, :, :, at].reshape(n_expert * tokens, width)
            value = jnp.dot(spr[...], right, preferred_element_type=F32)
            upd[:, at] = upd[:, at] + value if k else value
            if k == order[-1]:
                put(upd.at[:, at], upd_ref.at[:, at])

    second(order[0])
    second(order[1])
    for at, m in enumerate(order):
        update(m)
        if at + 2 < n_dp:
            second(order[at + 2])
    for j in range(pieces):

        @pl.when(inner)
        def _():
            over(j).wait_send()
            down(j).wait_send()

        @pl.when(jnp.logical_not(inner))
        def _():
            up(j).wait_send()

    for copy in sent:
        copy.wait_send()
    for copy in stored:
        copy.wait()


def fused_buffers(n_expert, n_dp, tokens, width, experts, slots, units, rank, top):
    cols = width // n_dp
    halves = ((2 * experts, rank // 2, units), BF16)
    return [
        ((n_dp, n_expert, tokens, cols), BF16),
        ((n_dp - 1, tokens, cols), BF16),
        ((experts, slots, units), BF16),
        ((n_expert, experts * rank, cols), BF16),
        ((n_dp, n_expert, 2 * top, tokens), F32),
        ((n_dp, experts, n_expert * tokens), F32),
        ((n_dp, experts, slots, n_expert * tokens), BF16),
        ((n_dp, n_expert * experts, tokens), F32),
        ((n_dp, n_expert, slots, tokens), BF16),
        ((2, n_expert, experts * rank, tokens), BF16),
        ((n_dp, n_expert, rank, slots), BF16),
        ((n_dp, n_expert, rank, slots), BF16),
        ((experts, slots, slots), BF16),
        halves,
        halves,
        halves,
        halves,
        ((experts, rank, 2 * rank), F32),
        ((n_dp, experts // 2, rank, 2 * slots), BF16),
        ((experts * rank, n_expert * tokens), BF16),
        ((experts, rank, units), F32),
        ((experts * rank, cols), F32),
    ]


def fused(grads, ids, probs, hidden, q, buffers):
    n_expert, n_dp = lax.axis_size("expert"), lax.axis_size("dp")
    experts, slots, units = hidden.shape
    rank = q.shape[0] // experts
    cols = q.shape[1] // n_dp
    chips = n_expert // 2
    long = max(math.isqrt(chips), chips // math.isqrt(chips))
    tags = n_dp + 1
    dma = pltpu.SemaphoreType.DMA
    vmem = pl.BlockSpec(memory_space=pltpu.VMEM)
    anywhere = pl.BlockSpec(memory_space=pl.ANY)
    return pl.pallas_call(
        functools.partial(fused_kernel, n_expert, n_dp),
        out_shape=(
            jax.ShapeDtypeStruct((experts, rank, units), F32),
            jax.ShapeDtypeStruct((experts * rank, cols), F32),
        ),
        in_specs=[anywhere, vmem, vmem, anywhere, anywhere],
        out_specs=(anywhere, anywhere),
        scratch_shapes=[pltpu.VMEM(*b) for b in buffers] + [
            pltpu.SemaphoreType.REGULAR, dma((2 + cols // 128,)), dma((n_dp + 1 + experts,)),
            dma((n_dp, n_expert)), dma((n_dp, n_expert)), dma((n_dp,)), dma((n_dp,)),
            dma((n_dp,)), dma((n_dp,)),
            dma((2, tags, long - 1)), dma((2, tags, long - 1)),
            dma((2, tags, long, long - 1)), dma((2, tags, long, long - 1)),
            dma((2, tags, long, long)), dma((2, tags, long, long)),
            dma((n_dp, n_expert)), dma((n_dp, n_expert)),
            dma((3, 2 * experts)), dma((3, 2 * experts)), dma((n_dp, 2)), dma((n_dp, 2)),
        ],
        compiler_params=pltpu.CompilerParams(
            collective_id=2, has_side_effects=True, vmem_limit_bytes=67043328
        ),
        name="fused",
    )(grads, ids, probs, hidden, q)


def local(out_grads, expert_ids, gate_probs, hidden_acts, q_previous):
    n_expert, n_dp = lax.axis_size("expert"), lax.axis_size("dp")
    experts, slots, units = hidden_acts.shape[1:]
    tokens, width = out_grads.shape[1:]
    rank = q_previous.shape[1]
    cols = width // n_dp
    buffers = fused_buffers(
        n_expert, n_dp, tokens, width, experts, slots, units, rank, expert_ids.shape[2]
    )
    held = sum(math.prod(shape) * jnp.dtype(kind).itemsize for shape, kind in buffers)
    if n_dp != 4 or held > 60 * 2**20:
        return spacious(out_grads, expert_ids, gate_probs, hidden_acts, q_previous)
    q = q_previous.reshape(experts * rank, width)
    basis, update = fused(out_grads[0], expert_ids[0].T, gate_probs[0].T, hidden_acts[0], q, buffers)
    return (basis, update.reshape(experts, rank, cols))


def spacious(out_grads, expert_ids, gate_probs, hidden_acts, q_previous):
    n_expert = lax.axis_size("expert")
    n_dp = lax.axis_size("dp")
    experts, slots, units = hidden_acts.shape[1:]
    capacity = slots // n_expert
    tokens, width = out_grads.shape[1:]
    top = expert_ids.shape[2]
    rank = q_previous.shape[1]
    cols = width // n_dp
    first = lax.axis_index("expert") * experts

    route = jnp.concatenate([expert_ids[0].astype(F32), gate_probs[0]], axis=1).T
    grads, route = gathered(out_grads[0], route)
    mine = (first + jnp.arange(experts)).astype(F32)[:, None]
    ids = route[:, :, :top].transpose(2, 0, 1, 3)[:, :, :, None, :]
    weight = route[:, :, top:].transpose(2, 0, 1, 3)[:, :, :, None, :]
    hit = ids == mine
    gate = jnp.sum(jnp.where(hit, weight, 0.0), axis=0)
    chosen = jnp.any(hit, axis=0)
    earlier = (jnp.arange(tokens)[:, None] < jnp.arange(tokens)[None, :]).astype(BF16)
    place = jnp.einsum("pbjt,tu->pbju", chosen.astype(BF16), earlier, preferred_element_type=F32)
    place = jnp.where(chosen, place, -1.0)
    pick = (place[:, :, :, None, :] == jnp.arange(capacity, dtype=F32)[:, None]).astype(BF16)

    q_part = lax.dynamic_slice_in_dim(q_previous, lax.axis_index("dp") * cols, cols, 2)
    mixed = jnp.einsum("jrd,bptd->jrbpt", q_part, grads, preferred_element_type=F32)
    scale = gate.transpose(2, 1, 0, 3)
    mixed = (mixed * scale[:, None]).astype(BF16)
    part = jnp.einsum("jrbpt,pbjct->pjrbc", mixed, pick, preferred_element_type=F32).astype(BF16)
    part = part.reshape(n_dp, experts, rank, slots)
    ortho, proj = factors(part, hidden_acts[0], n_dp)
    proj = proj.reshape(n_dp, experts, rank, n_expert, capacity)
    spread = jnp.einsum("pjrbc,pbjct->jrbpt", proj, pick, preferred_element_type=F32)
    spread = (spread * scale[:, None]).astype(BF16)
    q_update = jnp.einsum("jrbpt,bptd->jrd", spread, grads, preferred_element_type=F32)
    new_basis = ortho.astype(F32) * math.sqrt(units)
    return (new_basis, q_update)


def solution(mesh):
    return jax.shard_map(
        local,
        mesh=mesh,
        in_specs=(
            P("dp", "expert", None),
            P("dp", "expert", None),
            P("dp", "expert", None),
            P("dp", "expert", None, None),
            P("expert", None, None),
        ),
        out_specs=(P("expert", None, None), P("expert", None, "dp")),
        check_vma=False,
    )
```

```python
import functools
import math

import jax
import jax.numpy as jnp
from jax import lax
from jax.experimental import pallas as pl
from jax.experimental.pallas import tpu as pltpu
from jax.sharding import PartitionSpec as P

F32, BF16 = jnp.float32, jnp.bfloat16


MESH = pl.DeviceIdType.MESH


def orthonormal(value):
    rank = value[0].shape[0]
    rows = lax.broadcasted_iota(jnp.int32, (rank, 2 * rank), 0)
    cols = lax.broadcasted_iota(jnp.int32, (rank, 2 * rank), 1)
    eye = (cols == rows + rank).astype(F32)
    tables = []
    for one in value:
        doubled = jnp.concatenate([one, jnp.zeros_like(one)], axis=0)
        gram = lax.dot_general(
            one, doubled, (((1,), (1,)), ((), ())),
            precision=lax.Precision.HIGHEST, preferred_element_type=F32,
        )
        tables.append(gram + eye)
    for k in range(rank):
        for j, table in enumerate(tables):
            row = table[k : k + 1, :]
            pivot = lax.rsqrt(row[:, k : k + 1])
            scaled = row * pivot
            column = table[:, k : k + 1] * pivot
            table = jnp.where(rows > k, table - column * scaled, table)
            tables[j] = jnp.where(rows == k, scaled, table)
    return [
        jnp.dot(
            table[:, rank:], one, precision=lax.Precision.HIGHEST, preferred_element_type=F32
        )
        for table, one in zip(tables, value)
    ]


def factor_kernel(
    n, part_ref, hidden_ref, ortho_ref, proj_ref,
    hidden, got_part, fact, got_fact, load_sem, send_sem, recv_sem,
):
    me = lax.axis_index("dp")
    experts = hidden.shape[0]
    per = experts // n
    peers = [lax.rem(me + offset, n) for offset in range(1, n)]
    loads = []
    for j in range(experts):
        load = pltpu.make_async_copy(hidden_ref.at[j], hidden.at[j], load_sem.at[j])
        load.start()
        loads.append(load)
    barrier = pltpu.get_barrier_semaphore()
    for peer in peers:
        pl.semaphore_signal(barrier, inc=1, device_id={"dp": peer}, device_id_type=MESH)
    pl.semaphore_wait(barrier, n - 1)

    def push(phase, offset, source, target):
        copy = pltpu.make_async_remote_copy(
            src_ref=source,
            dst_ref=target,
            send_sem=send_sem.at[phase, offset],
            recv_sem=recv_sem.at[phase, offset],
            device_id={"dp": peers[offset]},
            device_id_type=MESH,
        )
        copy.start()
        return copy

    sent = [push(0, o, part_ref.at[peers[o]], got_part.at[o]) for o in range(n - 1)]
    for copy in sent:
        copy.wait()
    mixed = part_ref[me].astype(F32)
    for o in range(n - 1):
        mixed = mixed + got_part[o].astype(F32)
    mixed = mixed.astype(BF16)
    for load in loads:
        load.wait()
    rank = mixed.shape[1]
    for j in range(experts):
        fact[j] = jnp.dot(mixed[j], hidden[j], preferred_element_type=F32).astype(BF16)
    sent = [
        push(1, o, fact.at[pl.ds(peers[o] * per, per)], got_fact.at[o]) for o in range(n - 1)
    ]
    for copy in sent:
        copy.wait()
    share = []
    for i in range(per):
        total = fact[me * per + i].astype(F32)
        for o in range(n - 1):
            total = total + got_fact[o, i].astype(F32)
        share.append(total)
    for i, value in enumerate(orthonormal(share)):
        ortho_ref[me * per + i] = value.astype(BF16)
    mine = ortho_ref.at[pl.ds(me * per, per)]
    sent = [push(2, o, mine, mine) for o in range(n - 1)]

    def project(group):
        for i in range(per):
            j = group * per + i
            proj_ref[me, j] = lax.dot_general(
                ortho_ref[j], hidden[j], (((1,), (1,)), ((), ())), preferred_element_type=F32
            ).astype(BF16)

    project(me)
    for o in range(n - 1):
        sent[o].wait()
        project(lax.rem(me + n - 1 - o, n))
    sent = [push(3, o, proj_ref.at[me], proj_ref.at[me]) for o in range(n - 1)]
    for copy in sent:
        copy.wait()


def factors(part, hidden, n):
    experts, slots, units = hidden.shape
    rank = part.shape[2]
    per = experts // n
    vmem = pl.BlockSpec(memory_space=pltpu.VMEM)
    return pl.pallas_call(
        functools.partial(factor_kernel, n),
        out_shape=(
            jax.ShapeDtypeStruct((experts, rank, units), BF16),
            jax.ShapeDtypeStruct((n, experts, rank, slots), BF16),
        ),
        in_specs=[vmem, pl.BlockSpec(memory_space=pl.ANY)],
        out_specs=(vmem, vmem),
        scratch_shapes=[
            pltpu.VMEM((experts, slots, units), BF16),
            pltpu.VMEM((n - 1, experts, rank, slots), BF16),
            pltpu.VMEM((experts, rank, units), BF16),
            pltpu.VMEM((n - 1, per, rank, units), BF16),
            pltpu.SemaphoreType.DMA((experts,)),
            pltpu.SemaphoreType.DMA((4, n - 1)),
            pltpu.SemaphoreType.DMA((4, n - 1)),
        ],
        compiler_params=pltpu.CompilerParams(
            collective_id=0, has_side_effects=True, vmem_limit_bytes=40 * 2**20
        ),
        name="factors",
    )(part, hidden)


def gather_kernel(
    n_expert, n_dp, x_ref, route_ref, all_ref, routes_ref,
    route_send, route_recv, own_sem, z_send, z_recv, one_send, one_recv, two_send, two_recv, core_send, core_recv,
):
    me, z = lax.axis_index("expert"), lax.axis_index("dp")
    chips = n_expert // 2
    wide = math.isqrt(chips)
    sides = (wide, chips // wide)
    core, chip = lax.rem(me, 2), me // 2
    spot = (lax.rem(chip, wide), chip // wide)
    half, cols = x_ref.shape[0] // 2, all_ref.shape[3]

    def shifted(dim, by):
        return lax.rem(spot[dim] + by + sides[dim], sides[dim])

    def block(x, y, c):
        return (y * wide + x) * 2 + c

    def neighbour(dim, by):
        moved = shifted(dim, by)
        return block(moved, spot[1], core) if dim == 0 else block(spot[0], moved, core)

    def source(dim, first, second, c):
        x, y = (first, second) if dim == 0 else (second, first)
        return block(shifted(0, -x), shifted(1, -y), c)

    barrier = pltpu.get_barrier_semaphore()
    def greet(i, carry):
        pl.semaphore_signal(barrier, inc=1, device_id=other_of(i), device_id_type=MESH)
        return carry

    def other_of(i):
        return {
            "expert": lax.rem(me + lax.rem(i, n_expert), n_expert),
            "dp": lax.rem(z + i // n_expert, n_dp),
        }

    total = n_expert * n_dp
    lax.fori_loop(1, total, greet, 0)
    pl.semaphore_wait(barrier, total - 1)

    sent = []
    mine = routes_ref.at[z, me]
    routes_ref[z, me] = route_ref[...]

    def push(src, dst, send_sem, recv_sem, device):
        copy = pltpu.make_async_remote_copy(
            src_ref=src, dst_ref=dst, send_sem=send_sem, recv_sem=recv_sem,
            device_id=device, device_id_type=MESH,
        )
        copy.start()
        sent.append(copy)
        return copy

    def columns(r):
        return x_ref.at[:, pl.ds(pl.multiple_of(r * cols, 128), cols)]

    own = pltpu.make_async_copy(columns(z), all_ref.at[me, z], own_sem)
    own.start()
    arrive_z, arrive_one, arrive_two, arrive_core = {}, {}, {}, []
    for k in range(1, n_dp):
        to = lax.rem(z + k, n_dp)
        arrive_z[k] = push(
            columns(to), all_ref.at[me, z], z_send.at[k - 1], z_recv.at[k - 1], {"dp": to}
        )

    def tell(i, carry):
        pltpu.make_async_remote_copy(
            src_ref=route_ref, dst_ref=mine, send_sem=route_send.at[i],
            recv_sem=route_recv.at[i], device_id=other_of(i), device_id_type=MESH,
        ).start()
        return carry

    lax.fori_loop(1, total, tell, 0)

    def rows(b, k, h):
        return all_ref.at[b, lax.rem(z - k + n_dp, n_dp), pl.ds(h * half, half)]

    def swap(k, h, first, second):
        part = rows(source(h, first, second, core), k, h)
        at = (h, k, first, second)
        partner = {"expert": block(spot[0], spot[1], 1 - core)}
        arrive_core.append(push(part, part, core_send.at[at], core_recv.at[at], partner))

    def onward(k, h, first):
        part = rows(source(h, first, 0, core), k, h)
        for by in range(1, sides[1 - h]):
            at = (h, k, first, by - 1)
            arrive_two[at] = push(
                part, part, two_send.at[at], two_recv.at[at], {"expert": neighbour(1 - h, by)}
            )
        swap(k, h, first, 0)

    for k in range(n_dp + 2):
        if k < n_dp:
            if k:
                arrive_z[k].wait_recv()
            else:
                own.wait()
            for h in range(2):
                part = rows(me, k, h)
                for by in range(1, sides[h]):
                    at = (h, k, by - 1)
                    arrive_one[at] = push(
                        part, part, one_send.at[at], one_recv.at[at], {"expert": neighbour(h, by)}
                    )
            for h in range(2):
                onward(k, h, 0)
        if 0 <= k - 1 < n_dp:
            for h in range(2):
                for by in range(1, sides[h]):
                    arrive_one[(h, k - 1, by - 1)].wait_recv()
                    onward(k - 1, h, by)
        if 0 <= k - 2 < n_dp:
            for h in range(2):
                for first in range(sides[h]):
                    for by in range(1, sides[1 - h]):
                        arrive_two[(h, k - 2, first, by - 1)].wait_recv()
                        swap(k - 2, h, first, by)
    def told(i, carry):
        pltpu.make_async_remote_copy(
            src_ref=route_ref, dst_ref=mine, send_sem=route_send.at[i],
            recv_sem=route_recv.at[i], device_id=other_of(i), device_id_type=MESH,
        ).wait()
        return carry

    lax.fori_loop(1, total, told, 0)
    for copy in arrive_core:
        copy.wait_recv()
    for copy in sent:
        copy.wait_send()


def gathered(grads, route):
    n_expert, n_dp = lax.axis_size("expert"), lax.axis_size("dp")
    tokens, width = grads.shape
    long = max(math.isqrt(n_expert // 2), n_expert // 2 // math.isqrt(n_expert // 2))
    dma = pltpu.SemaphoreType.DMA
    return pl.pallas_call(
        functools.partial(gather_kernel, n_expert, n_dp),
        out_shape=(
            jax.ShapeDtypeStruct((n_expert, n_dp, tokens, width // n_dp), grads.dtype),
            jax.ShapeDtypeStruct((n_dp, n_expert, *route.shape), route.dtype),
        ),
        in_specs=[pl.BlockSpec(memory_space=pltpu.VMEM)] * 2,
        out_specs=(pl.BlockSpec(memory_space=pl.ANY), pl.BlockSpec(memory_space=pltpu.VMEM)),
        scratch_shapes=[
            dma((n_expert * n_dp,)), dma((n_expert * n_dp,)), dma(()), dma((n_dp - 1,)), dma((n_dp - 1,)),
            dma((2, n_dp, long)), dma((2, n_dp, long)),
            dma((2, n_dp, long, long)), dma((2, n_dp, long, long)),
            dma((2, n_dp, long, long)), dma((2, n_dp, long, long)),
        ],
        compiler_params=pltpu.CompilerParams(
            collective_id=1, has_side_effects=True, vmem_limit_bytes=56 * 2**20
        ),
        name="gather_rows",
    )(grads, route)


def fused_kernel(
    n_expert, n_dp, grads_ref, ids_ref, probs_ref, hidden_ref, q_ref, basis_ref, upd_ref,
    rep, own, hid, qall, routes, gate, pick, near_gate, near_pick, weighed, message, parts, spots,
    fact, got_up, got_cross, tot, gram, proj, spr,
    basis, upd, plane_sem, out_sem, load_sem, route_send, route_recv, far_send, far_recv, z_send, z_recv,
    hop_send, one_recv, two_recv, core_recv, part_send, part_recv,
    ring_send, ring_recv, proj_send, proj_recv,
):
    me, z = lax.axis_index("expert"), lax.axis_index("dp")
    chips = n_expert // 2
    wide = math.isqrt(chips)
    sides = (wide, chips // wide)
    core, chip = lax.rem(me, 2), me // 2
    spot = (lax.rem(chip, wide), chip // wide)
    tokens, cols = rep.shape[2:]
    experts, slots, units = hid.shape
    rank = 2 * fact.shape[1]
    cap = slots // n_expert
    top = routes.shape[2] // 2
    mate = z + 1 - 2 * lax.rem(z, 2)
    cross = n_dp - 1 - z
    replica = [z, cross, mate, lax.rem(z + 2, n_dp)]
    order = [0, 2, 1, 3]

    def shifted(dim, by):
        return lax.rem(spot[dim] + by + sides[dim], sides[dim])

    def block(x, y, c):
        return (y * wide + x) * 2 + c

    def neighbour(dim, by):
        moved = shifted(dim, by)
        return block(moved, spot[1], core) if dim == 0 else block(spot[0], moved, core)

    def source(dim, first, second, c):
        x, y = (first, second) if dim == 0 else (second, first)
        return block(shifted(0, -x), shifted(1, -y), c)

    def beside(i):
        return {"expert": lax.rem(me + i, n_expert)}

    def quarter(ref, at):
        return ref.at[:, pl.ds(pl.multiple_of(at * cols, 128), cols)]

    loads = []

    def load(src, dst, at=None):
        copy = pltpu.make_async_copy(src, dst, load_sem.at[len(loads) if at is None else at])
        copy.start()
        loads.append(copy)

    for m in (1, 3, 2):
        load(quarter(grads_ref, replica[m]), own.at[m - 1])
    load(quarter(q_ref, z), qall.at[me])
    load(quarter(grads_ref, z), rep.at[0, me])
    for j in range(experts):
        load(hidden_ref.at[j], hid.at[j], n_dp + 1)

    barrier = pltpu.get_barrier_semaphore()
    greeted = [{"dp": replica[m]} for m in range(1, n_dp)]
    greeted += [beside(i) for i in range(1, n_expert)]
    for peer in greeted:
        pl.semaphore_signal(barrier, inc=1, device_id=peer, device_id_type=MESH)
    routes[0, me] = jnp.concatenate([ids_ref[...].astype(F32), probs_ref[...]], axis=0)
    own_route = routes.at[0, me]
    pl.semaphore_wait(barrier, len(greeted))
    for m in range(1, n_dp):
        pl.semaphore_signal(
            plane_sem, inc=1, device_id={"dp": replica[m]}, device_id_type=MESH
        )

    def awaited(ref, sem):
        return pltpu.make_async_remote_copy(
            src_ref=ref, dst_ref=ref, send_sem=sem, recv_sem=sem,
            device_id={"dp": mate}, device_id_type=MESH,
        )

    def push(src, dst, send_sem, recv_sem, device):
        copy = pltpu.make_async_remote_copy(
            src_ref=src, dst_ref=dst, send_sem=send_sem, recv_sem=recv_sem,
            device_id=device, device_id_type=MESH,
        )
        copy.start()
        return copy

    told_far, arrive_z = {}, {}
    for m in (1, 3, 2):
        told_far[m] = push(
            own_route, routes.at[m, me], far_send, far_recv.at[m], {"dp": replica[m]}
        )
    for at, m in enumerate((1, 3, 2)):
        loads[at].wait()
        arrive_z[m] = push(
            own.at[m - 1], rep.at[m, me], z_send, z_recv.at[m], {"dp": replica[m]}
        )

    arrive_one, arrive_two = {}, {}

    def rows(b, k, h):
        whole = rep.at[k, b] if k < n_dp else qall.at[b]
        half = whole.shape[0] // 2
        return whole.at[pl.ds(h * half, half)]

    def swap(k, h, first, second):
        part = rows(source(h, first, second, core), k, h)
        partner = {"expert": block(spot[0], spot[1], 1 - core)}
        push(part, part, hop_send.at[k], core_recv.at[k], partner)

    def onward(k, h, first):
        part = rows(source(h, first, 0, core), k, h)
        for by in range(1, sides[1 - h]):
            at = (h, k, first, by - 1)
            arrive_two[at] = push(
                part, part, hop_send.at[k], two_recv.at[at], {"expert": neighbour(1 - h, by)}
            )
        swap(k, h, first, 0)

    def begin(k):
        for h in range(2):
            part = rows(me, k, h)
            for by in range(1, sides[h]):
                at = (h, k, by - 1)
                arrive_one[at] = push(
                    part, part, hop_send.at[k], one_recv.at[at], {"expert": neighbour(h, by)}
                )
        for h in range(2):
            onward(k, h, 0)

    def forward(k):
        for h in range(2):
            for by in range(1, sides[h]):
                arrive_one[h, k, by - 1].wait_recv()
                onward(k, h, by)

    def second(k):
        for h in range(2):
            for first in range(sides[h]):
                for by in range(1, sides[1 - h]):
                    arrive_two[h, k, first, by - 1].wait_recv()
                    swap(k, h, first, by)

    def landed(k):
        whole = rep.at[k] if k < n_dp else qall
        awaited(whole.at[pl.ds(0, chips)], core_recv.at[k]).wait_recv()

    def matched(table, first, count):
        ours = lax.broadcasted_iota(jnp.int32, (count, tokens), 0) + first
        ours = ours.astype(F32)
        value = jnp.zeros((count, tokens), F32)
        hit = jnp.zeros((count, tokens), F32)
        for t in range(top):
            same = table[t : t + 1, :] == ours
            value = jnp.where(same, table[top + t : top + t + 1, :], value)
            hit = jnp.where(same, 1.0, hit)
        return value, hit

    def positions(hits):
        before = lax.broadcasted_iota(jnp.int32, (tokens, tokens), 0)
        after = lax.broadcasted_iota(jnp.int32, (tokens, tokens), 1)
        earlier = jnp.where(before < after, 1.0, 0.0).astype(BF16)
        count = jnp.dot(hits.astype(BF16), earlier, preferred_element_type=F32)
        return jnp.where(hits > 0.5, count, -float(slots))

    def place_tokens(k):
        awaited(routes.at[k, pl.ds(0, n_expert - 1)], route_recv.at[k]).wait_recv()
        found = [matched(routes[k, b], me * experts, experts) for b in range(n_expert)]
        gate[k] = jnp.concatenate([value for value, _ in found], axis=1)
        count = positions(jnp.concatenate([hit for _, hit in found], axis=0))
        keys = [
            count[b * experts : (b + 1) * experts] + float(b * cap) for b in range(n_expert)
        ]
        key = jnp.concatenate(keys, axis=1).astype(jnp.int32)
        level = lax.broadcasted_iota(jnp.int32, (slots, n_expert * tokens), 0)
        for j in range(experts):
            pick[k, j] = jnp.where(level == key[j : j + 1, :], 1.0, 0.0).astype(BF16)

    def place_near(m):
        value, hit = matched(routes[m, me], 0, n_expert * experts)
        near_gate[m] = value
        key = positions(hit).astype(jnp.int32)
        level = lax.broadcasted_iota(jnp.int32, (cap, tokens), 0)
        for b in range(n_expert):
            rows_of = [
                jnp.where(level == key[b * experts + j : b * experts + j + 1, :], 1.0, 0.0)
                for j in range(experts)
            ]
            near_pick[m, b] = jnp.concatenate(rows_of, axis=0).astype(BF16)

    def folded(value, count, size):
        line = lax.broadcasted_iota(jnp.int32, (rank, value.shape[1]), 1)
        out = jnp.zeros((rank, value.shape[1]), F32)
        for j in range(count):
            mine = jnp.logical_and(line >= j * size, line < (j + 1) * size)
            out = jnp.where(mine, value[j * rank : (j + 1) * rank], out)
        return out

    def contract(ms):
        for i in range(n_expert):
            b = lax.rem(me + i, n_expert)
            near = jnp.concatenate([rep[m, me] for m in ms], axis=0)
            value = lax.dot_general(
                qall[b], near, (((1,), (1,)), ((), ())), preferred_element_type=F32
            )
            for at, m in enumerate(ms):
                scale = near_gate[m, pl.ds(pl.multiple_of(b * experts, experts), experts)]
                one = value[:, at * tokens : (at + 1) * tokens]
                one = one.reshape(experts, rank, tokens) * scale[:, None, :]
                weighed[at, i] = one.reshape(experts * rank, tokens).astype(BF16)
        for at, m in enumerate(ms):
            for i in range(n_expert):
                b = lax.rem(me + i, n_expert)
                value = lax.dot_general(
                    weighed[at, i], near_pick[m, b], (((1,), (1,)), ((), ())),
                    preferred_element_type=F32,
                )
                message[m, i] = folded(value, experts, cap).astype(BF16)
        for m in ms:
            for i in range(n_expert):
                if m == 0 and i == 0:
                    parts[0, me] = message[0, 0]
                    continue
                push(
                    message.at[m, i], parts.at[m, me],
                    part_send.at[min(m, 1)], part_recv.at[min(m, 1)],
                    {"expert": lax.rem(me + i, n_expert), "dp": replica[m]},
                )

    loads[3].wait()
    begin(n_dp)
    across = lax.broadcasted_iota(jnp.int32, (slots, slots), 0)
    along = lax.broadcasted_iota(jnp.int32, (slots, slots), 1)
    along = along - cap * (along // cap)
    for j in range(experts):
        spots[j] = jnp.where(across == along + j * cap, 1.0, 0.0).astype(BF16)
    loads[4].wait()
    pltpu.make_async_copy(hidden_ref, hid, load_sem.at[n_dp + 1]).wait()
    place_near(0)
    forward(n_dp)
    begin(0)
    for m in range(1, n_dp):
        told_far[m].wait_recv()
        place_near(m)
    second(n_dp)
    pl.semaphore_wait(plane_sem, n_dp - 1)
    arrive_z[2].wait_recv()
    landed(n_dp)
    contract((0, 2))
    arrive_z[1].wait_recv()
    contract((1,))
    forward(0)
    for m in order:
        for i in range(1, n_expert):
            push(routes.at[m, me], routes.at[m, me], route_send, route_recv.at[m], beside(i))
    arrive_z[3].wait_recv()
    contract((3,))
    for m in order[1:]:
        begin(m)

    inner = jnp.logical_or(z == 1, z == 2)

    def hop(kind, j, src, dst, to):
        return pltpu.make_async_remote_copy(
            src_ref=src.at[j], dst_ref=dst.at[j],
            send_sem=ring_send.at[kind], recv_sem=ring_recv.at[kind, j],
            device_id={"dp": to}, device_id_type=MESH,
        )

    def up(j):
        return hop(0, j, fact, got_up, mate)

    def over(j):
        return hop(1, j, fact, got_cross, cross)

    def down(j):
        return hop(2, j, tot, tot, mate)

    near_parts, far_parts = pl.ds(0, n_expert - 1), pl.ds(1, n_dp - 1)
    awaited(parts.at[0, near_parts], part_recv.at[0]).wait_recv()
    awaited(parts.at[far_parts], part_recv.at[1]).wait_recv()
    filled = []
    for b in range(n_expert):
        value = parts[0, b].astype(F32)
        for m in range(1, n_dp):
            value = value + parts[m, b].astype(F32)
        filled.append(value.astype(BF16))
    filled = jnp.concatenate(filled, axis=0)
    for j in range(experts):
        value = jnp.dot(filled, spots[j], preferred_element_type=F32)
        value = folded(value, n_expert, cap).astype(BF16)
        value = jnp.dot(value, hid[j], preferred_element_type=F32).astype(BF16)
        fact[2 * j : 2 * j + 2] = value.reshape(2, rank // 2, units)

        @pl.when(jnp.logical_not(inner))
        def _():
            up(2 * j).start()
            up(2 * j + 1).start()

    ahead = 3
    pieces = 2 * experts
    for step in range(pieces + ahead):
        if step < pieces:

            @pl.when(inner)
            def _():
                up(step).wait_recv()
                fact[step] = (fact[step].astype(F32) + got_up[step].astype(F32)).astype(BF16)
                over(step).start()

        if step >= ahead:
            j = step - ahead

            @pl.when(inner)
            def _():
                over(j).wait_recv()
                tot[j] = (fact[j].astype(F32) + got_cross[j].astype(F32)).astype(BF16)
                down(j).start()

        if step in (1, 3, 5, 7):
            place_tokens(order[step // 2])
        if step == 9:
            forward(2)
        if step == 13:
            forward(1)
        if step == 17:
            forward(3)

    shape = (rank, 2 * rank)
    eye = lax.broadcasted_iota(jnp.int32, shape, 1) == lax.broadcasted_iota(jnp.int32, shape, 0) + rank
    eye = jnp.where(eye, 1.0, 0.0)
    for j in range(experts):

        @pl.when(jnp.logical_not(inner))
        def _():
            down(2 * j).wait_recv()
            down(2 * j + 1).wait_recv()

        one = tot[2 * j : 2 * j + 2].reshape(rank, units)
        doubled = jnp.concatenate([one, jnp.zeros_like(one)], axis=0)
        gram[j] = eye + lax.dot_general(
            one, doubled, (((1,), (1,)), ((), ())), preferred_element_type=F32
        )

    table = [gram[:, k, :].T for k in range(rank)]
    for k in range(rank):
        row = table[k]
        scaled = row * (1.0 / row[k : k + 1, :])
        for i in range(k + 1, rank):
            table[i] = table[i] - row[i : i + 1, :] * scaled
        table[k] = row * lax.rsqrt(row[k : k + 1, :])
    for k in range(rank):
        gram[:, k, :] = table[k].T

    batch = experts // 2

    def put(src, dst, at):
        pltpu.make_async_copy(src, dst, out_sem.at[at]).start()

    for j in range(experts):
        inverse = gram[j][:, rank:]
        high = inverse.astype(BF16)
        low = (inverse - high.astype(F32)).astype(BF16)
        one = tot[2 * j : 2 * j + 2].reshape(rank, units)
        value = jnp.dot(high, one, preferred_element_type=F32)
        value = value + jnp.dot(low, one, preferred_element_type=F32)
        basis[j] = value * math.sqrt(units)
        value = value.astype(BF16)
        proj[0, j // 2, :, (j % 2) * slots : (j % 2 + 1) * slots] = lax.dot_general(
            value, hid[j], (((1,), (1,)), ((), ())), preferred_element_type=F32
        ).astype(BF16)
        if (j + 1) % batch == 0:
            g = j // batch
            put(basis.at[pl.ds(g * batch, batch)], basis_ref.at[pl.ds(g * batch, batch)], 0)
            part = pl.ds(g * batch // 2, batch // 2)
            for k in (3, 1, 2):
                push(
                    proj.at[0, part], proj.at[k, part],
                    proj_send, proj_recv.at[k], {"dp": replica[k]},
                )

    def update(k):
        if k:
            awaited(proj.at[k], proj_recv.at[k]).wait_recv()
        for j in range(experts):
            value = jnp.dot(
                proj[k, j // 2, :, (j % 2) * slots : (j % 2 + 1) * slots], pick[k, j],
                preferred_element_type=F32,
            )
            spr[j * rank : (j + 1) * rank] = (value * gate[k, j : j + 1, :]).astype(BF16)
        landed(k)
        width = 256 if cols % 256 == 0 else 128
        for c in range(cols // width):
            at = slice(c * width, (c + 1) * width)
            right = rep[k, :, :, at].reshape(n_expert * tokens, width)
            value = jnp.dot(spr[...], right, preferred_element_type=F32)
            upd[:, at] = upd[:, at] + value if k else value
            if k == order[-1]:
                put(upd.at[:, at], upd_ref.at[:, at], 1)

    second(order[0])
    second(order[1])
    for at, m in enumerate(order):
        update(m)
        if at + 2 < n_dp:
            second(order[at + 2])

    @pl.when(inner)
    def _():
        awaited(fact, ring_send.at[1]).wait_send()
        awaited(tot, ring_send.at[2]).wait_send()

    @pl.when(jnp.logical_not(inner))
    def _():
        awaited(fact, ring_send.at[0]).wait_send()

    for k in range(n_dp):
        awaited(rep.at[k, near_parts], hop_send.at[k]).wait_send()
    awaited(qall.at[near_parts], hop_send.at[n_dp]).wait_send()
    awaited(routes.at[:, near_parts], route_send).wait_send()
    awaited(routes.at[0, pl.ds(0, n_dp - 1)], far_send).wait_send()
    awaited(own, z_send).wait_send()
    awaited(message.at[0, near_parts], part_send.at[0]).wait_send()
    awaited(message.at[far_parts], part_send.at[1]).wait_send()
    awaited(proj.at[far_parts], proj_send).wait_send()
    pltpu.make_async_copy(basis, basis_ref, out_sem.at[0]).wait()
    pltpu.make_async_copy(upd, upd_ref, out_sem.at[1]).wait()


def fused_buffers(n_expert, n_dp, tokens, width, experts, slots, units, rank, top):
    cols = width // n_dp
    halves = ((2 * experts, rank // 2, units), BF16)
    return [
        ((n_dp, n_expert, tokens, cols), BF16),
        ((n_dp - 1, tokens, cols), BF16),
        ((experts, slots, units), BF16),
        ((n_expert, experts * rank, cols), BF16),
        ((n_dp, n_expert, 2 * top, tokens), F32),
        ((n_dp, experts, n_expert * tokens), F32),
        ((n_dp, experts, slots, n_expert * tokens), BF16),
        ((n_dp, n_expert * experts, tokens), F32),
        ((n_dp, n_expert, slots, tokens), BF16),
        ((2, n_expert, experts * rank, tokens), BF16),
        ((n_dp, n_expert, rank, slots), BF16),
        ((n_dp, n_expert, rank, slots), BF16),
        ((experts, slots, slots), BF16),
        halves,
        halves,
        halves,
        halves,
        ((experts, rank, 2 * rank), F32),
        ((n_dp, experts // 2, rank, 2 * slots), BF16),
        ((experts * rank, n_expert * tokens), BF16),
        ((experts, rank, units), F32),
        ((experts * rank, cols), F32),
    ]


def fused(grads, ids, probs, hidden, q, buffers):
    n_expert, n_dp = lax.axis_size("expert"), lax.axis_size("dp")
    experts, slots, units = hidden.shape
    rank = q.shape[0] // experts
    cols = q.shape[1] // n_dp
    chips = n_expert // 2
    long = max(math.isqrt(chips), chips // math.isqrt(chips))
    tags = n_dp + 1
    dma = pltpu.SemaphoreType.DMA
    vmem = pl.BlockSpec(memory_space=pltpu.VMEM)
    anywhere = pl.BlockSpec(memory_space=pl.ANY)
    return pl.pallas_call(
        functools.partial(fused_kernel, n_expert, n_dp),
        out_shape=(
            jax.ShapeDtypeStruct((experts, rank, units), F32),
            jax.ShapeDtypeStruct((experts * rank, cols), F32),
        ),
        in_specs=[anywhere, vmem, vmem, anywhere, anywhere],
        out_specs=(anywhere, anywhere),
        scratch_shapes=[pltpu.VMEM(*b) for b in buffers] + [
            pltpu.SemaphoreType.REGULAR, dma((2,)), dma((n_dp + 2,)),
            dma(()), dma((n_dp,)), dma(()), dma((n_dp,)), dma(()), dma((n_dp,)),
            dma((tags,)), dma((2, tags, long - 1)), dma((2, tags, long, long - 1)), dma((tags,)),
            dma((2,)), dma((2,)), dma((3,)), dma((3, 2 * experts)), dma(()), dma((n_dp,)),
        ],
        compiler_params=pltpu.CompilerParams(
            collective_id=2, has_side_effects=True, vmem_limit_bytes=67043328
        ),
        name="fused",
    )(grads, ids, probs, hidden, q)


def local(out_grads, expert_ids, gate_probs, hidden_acts, q_previous):
    n_expert, n_dp = lax.axis_size("expert"), lax.axis_size("dp")
    experts, slots, units = hidden_acts.shape[1:]
    tokens, width = out_grads.shape[1:]
    rank = q_previous.shape[1]
    cols = width // n_dp
    buffers = fused_buffers(
        n_expert, n_dp, tokens, width, experts, slots, units, rank, expert_ids.shape[2]
    )
    held = sum(math.prod(shape) * jnp.dtype(kind).itemsize for shape, kind in buffers)
    if n_dp != 4 or held > 60 * 2**20:
        return spacious(out_grads, expert_ids, gate_probs, hidden_acts, q_previous)
    q = q_previous.reshape(experts * rank, width)
    basis, update = fused(out_grads[0], expert_ids[0].T, gate_probs[0].T, hidden_acts[0], q, buffers)
    return (basis, update.reshape(experts, rank, cols))


def spacious(out_grads, expert_ids, gate_probs, hidden_acts, q_previous):
    n_expert = lax.axis_size("expert")
    n_dp = lax.axis_size("dp")
    experts, slots, units = hidden_acts.shape[1:]
    capacity = slots // n_expert
    tokens, width = out_grads.shape[1:]
    top = expert_ids.shape[2]
    rank = q_previous.shape[1]
    cols = width // n_dp
    first = lax.axis_index("expert") * experts

    route = jnp.concatenate([expert_ids[0].astype(F32), gate_probs[0]], axis=1).T
    grads, route = gathered(out_grads[0], route)
    mine = (first + jnp.arange(experts)).astype(F32)[:, None]
    ids = route[:, :, :top].transpose(2, 0, 1, 3)[:, :, :, None, :]
    weight = route[:, :, top:].transpose(2, 0, 1, 3)[:, :, :, None, :]
    hit = ids == mine
    gate = jnp.sum(jnp.where(hit, weight, 0.0), axis=0)
    chosen = jnp.any(hit, axis=0)
    earlier = (jnp.arange(tokens)[:, None] < jnp.arange(tokens)[None, :]).astype(BF16)
    place = jnp.einsum("pbjt,tu->pbju", chosen.astype(BF16), earlier, preferred_element_type=F32)
    place = jnp.where(chosen, place, -1.0)
    pick = (place[:, :, :, None, :] == jnp.arange(capacity, dtype=F32)[:, None]).astype(BF16)

    q_part = lax.dynamic_slice_in_dim(q_previous, lax.axis_index("dp") * cols, cols, 2)
    mixed = jnp.einsum("jrd,bptd->jrbpt", q_part, grads, preferred_element_type=F32)
    scale = gate.transpose(2, 1, 0, 3)
    mixed = (mixed * scale[:, None]).astype(BF16)
    part = jnp.einsum("jrbpt,pbjct->pjrbc", mixed, pick, preferred_element_type=F32).astype(BF16)
    part = part.reshape(n_dp, experts, rank, slots)
    ortho, proj = factors(part, hidden_acts[0], n_dp)
    proj = proj.reshape(n_dp, experts, rank, n_expert, capacity)
    spread = jnp.einsum("pjrbc,pbjct->jrbpt", proj, pick, preferred_element_type=F32)
    spread = (spread * scale[:, None]).astype(BF16)
    q_update = jnp.einsum("jrbpt,bptd->jrd", spread, grads, preferred_element_type=F32)
    new_basis = ortho.astype(F32) * math.sqrt(units)
    return (new_basis, q_update)


def solution(mesh):
    return jax.shard_map(
        local,
        mesh=mesh,
        in_specs=(
            P("dp", "expert", None),
            P("dp", "expert", None),
            P("dp", "expert", None),
            P("dp", "expert", None, None),
            P("expert", None, None),
        ),
        out_specs=(P("expert", None, None), P("expert", None, "dp")),
        check_vma=False,
    )
```

```python
import functools
import math

import jax
import jax.numpy as jnp
from jax import lax
from jax.experimental import pallas as pl
from jax.experimental.pallas import tpu as pltpu
from jax.sharding import PartitionSpec as P

F32, BF16 = jnp.float32, jnp.bfloat16


MESH = pl.DeviceIdType.MESH


def orthonormal(value):
    rank = value[0].shape[0]
    rows = lax.broadcasted_iota(jnp.int32, (rank, 2 * rank), 0)
    cols = lax.broadcasted_iota(jnp.int32, (rank, 2 * rank), 1)
    eye = (cols == rows + rank).astype(F32)
    tables = []
    for one in value:
        doubled = jnp.concatenate([one, jnp.zeros_like(one)], axis=0)
        gram = lax.dot_general(
            one, doubled, (((1,), (1,)), ((), ())),
            precision=lax.Precision.HIGHEST, preferred_element_type=F32,
        )
        tables.append(gram + eye)
    for k in range(rank):
        for j, table in enumerate(tables):
            row = table[k : k + 1, :]
            pivot = lax.rsqrt(row[:, k : k + 1])
            scaled = row * pivot
            column = table[:, k : k + 1] * pivot
            table = jnp.where(rows > k, table - column * scaled, table)
            tables[j] = jnp.where(rows == k, scaled, table)
    return [
        jnp.dot(
            table[:, rank:], one, precision=lax.Precision.HIGHEST, preferred_element_type=F32
        )
        for table, one in zip(tables, value)
    ]


def factor_kernel(
    n, part_ref, hidden_ref, ortho_ref, proj_ref,
    hidden, got_part, fact, got_fact, load_sem, send_sem, recv_sem,
):
    me = lax.axis_index("dp")
    experts = hidden.shape[0]
    per = experts // n
    peers = [lax.rem(me + offset, n) for offset in range(1, n)]
    loads = []
    for j in range(experts):
        load = pltpu.make_async_copy(hidden_ref.at[j], hidden.at[j], load_sem.at[j])
        load.start()
        loads.append(load)
    barrier = pltpu.get_barrier_semaphore()
    for peer in peers:
        pl.semaphore_signal(barrier, inc=1, device_id={"dp": peer}, device_id_type=MESH)
    pl.semaphore_wait(barrier, n - 1)

    def push(phase, offset, source, target):
        copy = pltpu.make_async_remote_copy(
            src_ref=source,
            dst_ref=target,
            send_sem=send_sem.at[phase, offset],
            recv_sem=recv_sem.at[phase, offset],
            device_id={"dp": peers[offset]},
            device_id_type=MESH,
        )
        copy.start()
        return copy

    sent = [push(0, o, part_ref.at[peers[o]], got_part.at[o]) for o in range(n - 1)]
    for copy in sent:
        copy.wait()
    mixed = part_ref[me].astype(F32)
    for o in range(n - 1):
        mixed = mixed + got_part[o].astype(F32)
    mixed = mixed.astype(BF16)
    for load in loads:
        load.wait()
    rank = mixed.shape[1]
    for j in range(experts):
        fact[j] = jnp.dot(mixed[j], hidden[j], preferred_element_type=F32).astype(BF16)
    sent = [
        push(1, o, fact.at[pl.ds(peers[o] * per, per)], got_fact.at[o]) for o in range(n - 1)
    ]
    for copy in sent:
        copy.wait()
    share = []
    for i in range(per):
        total = fact[me * per + i].astype(F32)
        for o in range(n - 1):
            total = total + got_fact[o, i].astype(F32)
        share.append(total)
    for i, value in enumerate(orthonormal(share)):
        ortho_ref[me * per + i] = value.astype(BF16)
    mine = ortho_ref.at[pl.ds(me * per, per)]
    sent = [push(2, o, mine, mine) for o in range(n - 1)]

    def project(group):
        for i in range(per):
            j = group * per + i
            proj_ref[me, j] = lax.dot_general(
                ortho_ref[j], hidden[j], (((1,), (1,)), ((), ())), preferred_element_type=F32
            ).astype(BF16)

    project(me)
    for o in range(n - 1):
        sent[o].wait()
        project(lax.rem(me + n - 1 - o, n))
    sent = [push(3, o, proj_ref.at[me], proj_ref.at[me]) for o in range(n - 1)]
    for copy in sent:
        copy.wait()


def factors(part, hidden, n):
    experts, slots, units = hidden.shape
    rank = part.shape[2]
    per = experts // n
    vmem = pl.BlockSpec(memory_space=pltpu.VMEM)
    return pl.pallas_call(
        functools.partial(factor_kernel, n),
        out_shape=(
            jax.ShapeDtypeStruct((experts, rank, units), BF16),
            jax.ShapeDtypeStruct((n, experts, rank, slots), BF16),
        ),
        in_specs=[vmem, pl.BlockSpec(memory_space=pl.ANY)],
        out_specs=(vmem, vmem),
        scratch_shapes=[
            pltpu.VMEM((experts, slots, units), BF16),
            pltpu.VMEM((n - 1, experts, rank, slots), BF16),
            pltpu.VMEM((experts, rank, units), BF16),
            pltpu.VMEM((n - 1, per, rank, units), BF16),
            pltpu.SemaphoreType.DMA((experts,)),
            pltpu.SemaphoreType.DMA((4, n - 1)),
            pltpu.SemaphoreType.DMA((4, n - 1)),
        ],
        compiler_params=pltpu.CompilerParams(
            collective_id=0, has_side_effects=True, vmem_limit_bytes=40 * 2**20
        ),
        name="factors",
    )(part, hidden)


def gather_kernel(
    n_expert, n_dp, x_ref, route_ref, all_ref, routes_ref,
    route_send, route_recv, own_sem, z_send, z_recv, one_send, one_recv, two_send, two_recv, core_send, core_recv,
):
    me, z = lax.axis_index("expert"), lax.axis_index("dp")
    chips = n_expert // 2
    wide = math.isqrt(chips)
    sides = (wide, chips // wide)
    core, chip = lax.rem(me, 2), me // 2
    spot = (lax.rem(chip, wide), chip // wide)
    half, cols = x_ref.shape[0] // 2, all_ref.shape[3]

    def shifted(dim, by):
        return lax.rem(spot[dim] + by + sides[dim], sides[dim])

    def block(x, y, c):
        return (y * wide + x) * 2 + c

    def neighbour(dim, by):
        moved = shifted(dim, by)
        return block(moved, spot[1], core) if dim == 0 else block(spot[0], moved, core)

    def source(dim, first, second, c):
        x, y = (first, second) if dim == 0 else (second, first)
        return block(shifted(0, -x), shifted(1, -y), c)

    barrier = pltpu.get_barrier_semaphore()
    def greet(i, carry):
        pl.semaphore_signal(barrier, inc=1, device_id=other_of(i), device_id_type=MESH)
        return carry

    def other_of(i):
        return {
            "expert": lax.rem(me + lax.rem(i, n_expert), n_expert),
            "dp": lax.rem(z + i // n_expert, n_dp),
        }

    total = n_expert * n_dp
    lax.fori_loop(1, total, greet, 0)
    pl.semaphore_wait(barrier, total - 1)

    sent = []
    mine = routes_ref.at[z, me]
    routes_ref[z, me] = route_ref[...]

    def push(src, dst, send_sem, recv_sem, device):
        copy = pltpu.make_async_remote_copy(
            src_ref=src, dst_ref=dst, send_sem=send_sem, recv_sem=recv_sem,
            device_id=device, device_id_type=MESH,
        )
        copy.start()
        sent.append(copy)
        return copy

    def columns(r):
        return x_ref.at[:, pl.ds(pl.multiple_of(r * cols, 128), cols)]

    own = pltpu.make_async_copy(columns(z), all_ref.at[me, z], own_sem)
    own.start()
    arrive_z, arrive_one, arrive_two, arrive_core = {}, {}, {}, []
    for k in range(1, n_dp):
        to = lax.rem(z + k, n_dp)
        arrive_z[k] = push(
            columns(to), all_ref.at[me, z], z_send.at[k - 1], z_recv.at[k - 1], {"dp": to}
        )

    def tell(i, carry):
        pltpu.make_async_remote_copy(
            src_ref=route_ref, dst_ref=mine, send_sem=route_send.at[i],
            recv_sem=route_recv.at[i], device_id=other_of(i), device_id_type=MESH,
        ).start()
        return carry

    lax.fori_loop(1, total, tell, 0)

    def rows(b, k, h):
        return all_ref.at[b, lax.rem(z - k + n_dp, n_dp), pl.ds(h * half, half)]

    def swap(k, h, first, second):
        part = rows(source(h, first, second, core), k, h)
        at = (h, k, first, second)
        partner = {"expert": block(spot[0], spot[1], 1 - core)}
        arrive_core.append(push(part, part, core_send.at[at], core_recv.at[at], partner))

    def onward(k, h, first):
        part = rows(source(h, first, 0, core), k, h)
        for by in range(1, sides[1 - h]):
            at = (h, k, first, by - 1)
            arrive_two[at] = push(
                part, part, two_send.at[at], two_recv.at[at], {"expert": neighbour(1 - h, by)}
            )
        swap(k, h, first, 0)

    for k in range(n_dp + 2):
        if k < n_dp:
            if k:
                arrive_z[k].wait_recv()
            else:
                own.wait()
            for h in range(2):
                part = rows(me, k, h)
                for by in range(1, sides[h]):
                    at = (h, k, by - 1)
                    arrive_one[at] = push(
                        part, part, one_send.at[at], one_recv.at[at], {"expert": neighbour(h, by)}
                    )
            for h in range(2):
                onward(k, h, 0)
        if 0 <= k - 1 < n_dp:
            for h in range(2):
                for by in range(1, sides[h]):
                    arrive_one[(h, k - 1, by - 1)].wait_recv()
                    onward(k - 1, h, by)
        if 0 <= k - 2 < n_dp:
            for h in range(2):
                for first in range(sides[h]):
                    for by in range(1, sides[1 - h]):
                        arrive_two[(h, k - 2, first, by - 1)].wait_recv()
                        swap(k - 2, h, first, by)
    def told(i, carry):
        pltpu.make_async_remote_copy(
            src_ref=route_ref, dst_ref=mine, send_sem=route_send.at[i],
            recv_sem=route_recv.at[i], device_id=other_of(i), device_id_type=MESH,
        ).wait()
        return carry

    lax.fori_loop(1, total, told, 0)
    for copy in arrive_core:
        copy.wait_recv()
    for copy in sent:
        copy.wait_send()


def gathered(grads, route):
    n_expert, n_dp = lax.axis_size("expert"), lax.axis_size("dp")
    tokens, width = grads.shape
    long = max(math.isqrt(n_expert // 2), n_expert // 2 // math.isqrt(n_expert // 2))
    dma = pltpu.SemaphoreType.DMA
    return pl.pallas_call(
        functools.partial(gather_kernel, n_expert, n_dp),
        out_shape=(
            jax.ShapeDtypeStruct((n_expert, n_dp, tokens, width // n_dp), grads.dtype),
            jax.ShapeDtypeStruct((n_dp, n_expert, *route.shape), route.dtype),
        ),
        in_specs=[pl.BlockSpec(memory_space=pltpu.VMEM)] * 2,
        out_specs=(pl.BlockSpec(memory_space=pl.ANY), pl.BlockSpec(memory_space=pltpu.VMEM)),
        scratch_shapes=[
            dma((n_expert * n_dp,)), dma((n_expert * n_dp,)), dma(()), dma((n_dp - 1,)), dma((n_dp - 1,)),
            dma((2, n_dp, long)), dma((2, n_dp, long)),
            dma((2, n_dp, long, long)), dma((2, n_dp, long, long)),
            dma((2, n_dp, long, long)), dma((2, n_dp, long, long)),
        ],
        compiler_params=pltpu.CompilerParams(
            collective_id=1, has_side_effects=True, vmem_limit_bytes=56 * 2**20
        ),
        name="gather_rows",
    )(grads, route)


def fused_kernel(
    n_expert, n_dp, grads_ref, ids_ref, probs_ref, hidden_ref, q_ref, basis_ref, upd_ref,
    rep, own, hid, qall, routes, gate, pick, near_gate, near_pick, weighed, message, parts, spots,
    fact, got_up, got_cross, tot, gram, proj, spr,
    basis, upd, plane_sem, out_sem, load_sem, route_send, route_recv, far_send, far_recv, z_send, z_recv,
    hop_send, one_recv, two_recv, core_recv, part_send, part_recv,
    ring_send, ring_recv, proj_send, proj_recv,
):
    me, z = lax.axis_index("expert"), lax.axis_index("dp")
    chips = n_expert // 2
    wide = math.isqrt(chips)
    sides = (wide, chips // wide)
    core, chip = lax.rem(me, 2), me // 2
    spot = (lax.rem(chip, wide), chip // wide)
    tokens, cols = rep.shape[2:]
    experts, slots, units = hid.shape
    rank = 2 * fact.shape[1]
    cap = slots // n_expert
    top = routes.shape[2] // 2
    mate = z + 1 - 2 * lax.rem(z, 2)
    cross = n_dp - 1 - z
    replica = [z, cross, mate, lax.rem(z + 2, n_dp)]
    order = [0, 2, 1, 3]

    def shifted(dim, by):
        return lax.rem(spot[dim] + by + sides[dim], sides[dim])

    def block(x, y, c):
        return (y * wide + x) * 2 + c

    def neighbour(dim, by):
        moved = shifted(dim, by)
        return block(moved, spot[1], core) if dim == 0 else block(spot[0], moved, core)

    def source(dim, first, second, c):
        x, y = (first, second) if dim == 0 else (second, first)
        return block(shifted(0, -x), shifted(1, -y), c)

    def beside(i):
        return {"expert": lax.rem(me + i, n_expert)}

    def quarter(ref, at):
        return ref.at[:, pl.ds(pl.multiple_of(at * cols, 128), cols)]

    loads = []

    def load(src, dst, at=None):
        copy = pltpu.make_async_copy(src, dst, load_sem.at[len(loads) if at is None else at])
        copy.start()
        loads.append(copy)

    for m in (1, 3, 2):
        load(quarter(grads_ref, replica[m]), own.at[m - 1])
    load(quarter(q_ref, z), qall.at[me])
    load(quarter(grads_ref, z), rep.at[0, me])
    for j in range(experts):
        load(hidden_ref.at[j], hid.at[j], n_dp + 1)

    barrier = pltpu.get_barrier_semaphore()
    greeted = [{"dp": replica[m]} for m in range(1, n_dp)]
    greeted += [beside(i) for i in range(1, n_expert)]
    for peer in greeted:
        pl.semaphore_signal(barrier, inc=1, device_id=peer, device_id_type=MESH)
    routes[0, me] = jnp.concatenate([ids_ref[...].astype(F32), probs_ref[...]], axis=0)
    own_route = routes.at[0, me]
    pl.semaphore_wait(barrier, len(greeted))
    for m in range(1, n_dp):
        pl.semaphore_signal(
            plane_sem, inc=1, device_id={"dp": replica[m]}, device_id_type=MESH
        )

    def awaited(ref, sem):
        return pltpu.make_async_remote_copy(
            src_ref=ref, dst_ref=ref, send_sem=sem, recv_sem=sem,
            device_id={"dp": mate}, device_id_type=MESH,
        )

    def push(src, dst, send_sem, recv_sem, device):
        copy = pltpu.make_async_remote_copy(
            src_ref=src, dst_ref=dst, send_sem=send_sem, recv_sem=recv_sem,
            device_id=device, device_id_type=MESH,
        )
        copy.start()
        return copy

    told_far, arrive_z = {}, {}
    for m in (1, 3, 2):
        told_far[m] = push(
            own_route, routes.at[m, me], far_send, far_recv.at[m], {"dp": replica[m]}
        )
    for at, m in enumerate((1, 3, 2)):
        loads[at].wait()
        arrive_z[m] = push(
            own.at[m - 1], rep.at[m, me], z_send, z_recv.at[m], {"dp": replica[m]}
        )

    arrive_one, arrive_two = {}, {}

    def rows(b, k, h):
        whole = rep.at[k, b] if k < n_dp else qall.at[b]
        half = whole.shape[0] // 2
        return whole.at[pl.ds(h * half, half)]

    def swap(k, h, first, second):
        part = rows(source(h, first, second, core), k, h)
        partner = {"expert": block(spot[0], spot[1], 1 - core)}
        push(part, part, hop_send.at[k], core_recv.at[k], partner)

    def onward(k, h, first):
        part = rows(source(h, first, 0, core), k, h)
        for by in range(1, sides[1 - h]):
            at = (h, k, first, by - 1)
            arrive_two[at] = push(
                part, part, hop_send.at[k], two_recv.at[at], {"expert": neighbour(1 - h, by)}
            )
        swap(k, h, first, 0)

    def begin(k):
        for h in range(2):
            part = rows(me, k, h)
            for by in range(1, sides[h]):
                at = (h, k, by - 1)
                arrive_one[at] = push(
                    part, part, hop_send.at[k], one_recv.at[at], {"expert": neighbour(h, by)}
                )
        for h in range(2):
            onward(k, h, 0)

    def forward(k):
        for h in range(2):
            for by in range(1, sides[h]):
                arrive_one[h, k, by - 1].wait_recv()
                onward(k, h, by)

    def second(k):
        for h in range(2):
            for first in range(sides[h]):
                for by in range(1, sides[1 - h]):
                    arrive_two[h, k, first, by - 1].wait_recv()
                    swap(k, h, first, by)

    def landed(k):
        whole = rep.at[k] if k < n_dp else qall
        awaited(whole.at[pl.ds(0, chips)], core_recv.at[k]).wait_recv()

    def matched(table, first, count):
        ours = lax.broadcasted_iota(jnp.int32, (count, tokens), 0) + first
        ours = ours.astype(F32)
        value = jnp.zeros((count, tokens), F32)
        hit = jnp.zeros((count, tokens), F32)
        for t in range(top):
            same = table[t : t + 1, :] == ours
            value = jnp.where(same, table[top + t : top + t + 1, :], value)
            hit = jnp.where(same, 1.0, hit)
        return value, hit

    def positions(hits):
        before = lax.broadcasted_iota(jnp.int32, (tokens, tokens), 0)
        after = lax.broadcasted_iota(jnp.int32, (tokens, tokens), 1)
        earlier = jnp.where(before < after, 1.0, 0.0).astype(BF16)
        count = jnp.dot(hits.astype(BF16), earlier, preferred_element_type=F32)
        return jnp.where(hits > 0.5, count, -float(slots))

    def place_tokens(k):
        awaited(routes.at[k, pl.ds(0, n_expert - 1)], route_recv.at[k]).wait_recv()
        found = [matched(routes[k, b], me * experts, experts) for b in range(n_expert)]
        gate[k] = jnp.concatenate([value for value, _ in found], axis=1)
        count = positions(jnp.concatenate([hit for _, hit in found], axis=0))
        keys = [
            count[b * experts : (b + 1) * experts] + float(b * cap) for b in range(n_expert)
        ]
        key = jnp.concatenate(keys, axis=1).astype(jnp.int32)
        level = lax.broadcasted_iota(jnp.int32, (slots, n_expert * tokens), 0)
        for j in range(experts):
            pick[k, j] = jnp.where(level == key[j : j + 1, :], 1.0, 0.0).astype(BF16)

    def place_near(m):
        value, hit = matched(routes[m, me], 0, n_expert * experts)
        near_gate[m] = value
        key = positions(hit).astype(jnp.int32)
        level = lax.broadcasted_iota(jnp.int32, (cap, tokens), 0)
        for b in range(n_expert):
            rows_of = [
                jnp.where(level == key[b * experts + j : b * experts + j + 1, :], 1.0, 0.0)
                for j in range(experts)
            ]
            near_pick[m, b] = jnp.concatenate(rows_of, axis=0).astype(BF16)

    def folded(value, count, size):
        line = lax.broadcasted_iota(jnp.int32, (rank, value.shape[1]), 1)
        out = jnp.zeros((rank, value.shape[1]), F32)
        for j in range(count):
            mine = jnp.logical_and(line >= j * size, line < (j + 1) * size)
            out = jnp.where(mine, value[j * rank : (j + 1) * rank], out)
        return out

    packs = message.shape[3] != slots
    edge = slots // 128 * 128

    def packed(value):
        if not packs:
            return value
        tail = value[:, edge:]
        tail = jnp.concatenate([tail[: rank // 2], tail[rank // 2 :]], axis=1)
        return jnp.concatenate([value[:, :edge], tail], axis=0)

    def unpacked(value):
        if not packs:
            return value
        tail = value[rank:]
        tail = jnp.concatenate([tail[:, : edge // 2], tail[:, edge // 2 :]], axis=0)
        return jnp.concatenate([value[:rank], tail], axis=1)

    def contract(ms):
        for i in range(n_expert):
            b = lax.rem(me + i, n_expert)
            near = jnp.concatenate([rep[m, me] for m in ms], axis=0)
            value = lax.dot_general(
                qall[b], near, (((1,), (1,)), ((), ())), preferred_element_type=F32
            )
            for at, m in enumerate(ms):
                scale = near_gate[m, pl.ds(pl.multiple_of(b * experts, experts), experts)]
                one = value[:, at * tokens : (at + 1) * tokens]
                one = one.reshape(experts, rank, tokens) * scale[:, None, :]
                weighed[at, i] = one.reshape(experts * rank, tokens).astype(BF16)
        for at, m in enumerate(ms):
            for i in range(n_expert):
                b = lax.rem(me + i, n_expert)
                value = lax.dot_general(
                    weighed[at, i], near_pick[m, b], (((1,), (1,)), ((), ())),
                    preferred_element_type=F32,
                )
                message[m, i] = packed(folded(value, experts, cap)).astype(BF16)
        for m in ms:
            for i in range(n_expert):
                if m == 0 and i == 0:
                    parts[0, me] = message[0, 0]
                    continue
                push(
                    message.at[m, i], parts.at[m, me],
                    part_send.at[min(m, 1)], part_recv.at[min(m, 1)],
                    {"expert": lax.rem(me + i, n_expert), "dp": replica[m]},
                )

    loads[3].wait()
    begin(n_dp)
    across = lax.broadcasted_iota(jnp.int32, (slots, slots), 0)
    along = lax.broadcasted_iota(jnp.int32, (slots, slots), 1)
    along = along - cap * (along // cap)
    for j in range(experts):
        spots[j] = jnp.where(across == along + j * cap, 1.0, 0.0).astype(BF16)
    loads[4].wait()
    pltpu.make_async_copy(hidden_ref, hid, load_sem.at[n_dp + 1]).wait()
    place_near(0)
    forward(n_dp)
    begin(0)
    for m in range(1, n_dp):
        told_far[m].wait_recv()
        place_near(m)
    second(n_dp)
    pl.semaphore_wait(plane_sem, n_dp - 1)
    arrive_z[2].wait_recv()
    landed(n_dp)
    contract((0, 2))
    arrive_z[1].wait_recv()
    contract((1,))
    forward(0)
    for m in order:
        for i in range(1, n_expert):
            push(routes.at[m, me], routes.at[m, me], route_send, route_recv.at[m], beside(i))
    arrive_z[3].wait_recv()
    contract((3,))
    for m in order[1:]:
        begin(m)

    inner = jnp.logical_or(z == 1, z == 2)

    def hop(kind, j, src, dst, to):
        return pltpu.make_async_remote_copy(
            src_ref=src.at[j], dst_ref=dst.at[j],
            send_sem=ring_send.at[kind], recv_sem=ring_recv.at[kind, j],
            device_id={"dp": to}, device_id_type=MESH,
        )

    def up(j):
        return hop(0, j, fact, got_up, mate)

    def over(j):
        return hop(1, j, fact, got_cross, cross)

    def down(j):
        return hop(2, j, tot, tot, mate)

    near_parts, far_parts = pl.ds(0, n_expert - 1), pl.ds(1, n_dp - 1)
    awaited(parts.at[0, near_parts], part_recv.at[0]).wait_recv()
    awaited(parts.at[far_parts], part_recv.at[1]).wait_recv()
    filled = []
    for b in range(n_expert):
        value = parts[0, b].astype(F32)
        for m in range(1, n_dp):
            value = value + parts[m, b].astype(F32)
        filled.append(unpacked(value).astype(BF16))
    filled = jnp.concatenate(filled, axis=0)
    for j in range(experts):
        value = jnp.dot(filled, spots[j], preferred_element_type=F32)
        value = folded(value, n_expert, cap).astype(BF16)
        value = jnp.dot(value, hid[j], preferred_element_type=F32).astype(BF16)
        fact[2 * j : 2 * j + 2] = value.reshape(2, rank // 2, units)

        @pl.when(jnp.logical_not(inner))
        def _():
            up(2 * j).start()
            up(2 * j + 1).start()

    ahead = 3
    pieces = 2 * experts
    for step in range(pieces + ahead):
        if step < pieces:

            @pl.when(inner)
            def _():
                up(step).wait_recv()
                fact[step] = (fact[step].astype(F32) + got_up[step].astype(F32)).astype(BF16)
                over(step).start()

        if step >= ahead:
            j = step - ahead

            @pl.when(inner)
            def _():
                over(j).wait_recv()
                tot[j] = (fact[j].astype(F32) + got_cross[j].astype(F32)).astype(BF16)
                down(j).start()

        if step in (1, 3, 5, 7):
            place_tokens(order[step // 2])
        if step == 9:
            forward(2)
        if step == 13:
            forward(1)
        if step == 17:
            forward(3)

    shape = (rank, 2 * rank)
    eye = lax.broadcasted_iota(jnp.int32, shape, 1) == lax.broadcasted_iota(jnp.int32, shape, 0) + rank
    eye = jnp.where(eye, 1.0, 0.0)
    for j in range(experts):

        @pl.when(jnp.logical_not(inner))
        def _():
            down(2 * j).wait_recv()
            down(2 * j + 1).wait_recv()

        one = tot[2 * j : 2 * j + 2].reshape(rank, units)
        doubled = jnp.concatenate([one, jnp.zeros_like(one)], axis=0)
        gram[j] = eye + lax.dot_general(
            one, doubled, (((1,), (1,)), ((), ())), preferred_element_type=F32
        )

    table = [gram[:, k, :].T for k in range(rank)]
    for k in range(rank):
        row = table[k]
        scaled = row * (1.0 / row[k : k + 1, :])
        for i in range(k + 1, rank):
            table[i] = table[i] - row[i : i + 1, :] * scaled
        table[k] = row * lax.rsqrt(row[k : k + 1, :])
    for k in range(rank):
        gram[:, k, :] = table[k].T

    batch = experts // 2

    def put(src, dst, at):
        pltpu.make_async_copy(src, dst, out_sem.at[at]).start()

    for j in range(experts):
        inverse = gram[j][:, rank:]
        high = inverse.astype(BF16)
        low = (inverse - high.astype(F32)).astype(BF16)
        one = tot[2 * j : 2 * j + 2].reshape(rank, units)
        value = jnp.dot(high, one, preferred_element_type=F32)
        value = value + jnp.dot(low, one, preferred_element_type=F32)
        basis[j] = value * math.sqrt(units)
        value = value.astype(BF16)
        proj[0, j // 2, :, (j % 2) * slots : (j % 2 + 1) * slots] = lax.dot_general(
            value, hid[j], (((1,), (1,)), ((), ())), preferred_element_type=F32
        ).astype(BF16)
        if (j + 1) % batch == 0:
            g = j // batch
            put(basis.at[pl.ds(g * batch, batch)], basis_ref.at[pl.ds(g * batch, batch)], 0)
            part = pl.ds(g * batch // 2, batch // 2)
            for k in (3, 1, 2):
                push(
                    proj.at[0, part], proj.at[k, part],
                    proj_send, proj_recv.at[k], {"dp": replica[k]},
                )

    def update(k):
        if k:
            awaited(proj.at[k], proj_recv.at[k]).wait_recv()
        for j in range(experts):
            value = jnp.dot(
                proj[k, j // 2, :, (j % 2) * slots : (j % 2 + 1) * slots], pick[k, j],
                preferred_element_type=F32,
            )
            spr[j * rank : (j + 1) * rank] = (value * gate[k, j : j + 1, :]).astype(BF16)
        landed(k)
        width = 256 if cols % 256 == 0 else 128
        for c in range(cols // width):
            at = slice(c * width, (c + 1) * width)
            right = rep[k, :, :, at].reshape(n_expert * tokens, width)
            value = jnp.dot(spr[...], right, preferred_element_type=F32)
            upd[:, at] = upd[:, at] + value if k else value
            if k == order[-1]:
                put(upd.at[:, at], upd_ref.at[:, at], 1)

    second(order[0])
    second(order[1])
    for at, m in enumerate(order):
        update(m)
        if at + 2 < n_dp:
            second(order[at + 2])

    @pl.when(inner)
    def _():
        awaited(fact, ring_send.at[1]).wait_send()
        awaited(tot, ring_send.at[2]).wait_send()

    @pl.when(jnp.logical_not(inner))
    def _():
        awaited(fact, ring_send.at[0]).wait_send()

    for k in range(n_dp):
        awaited(rep.at[k, near_parts], hop_send.at[k]).wait_send()
    awaited(qall.at[near_parts], hop_send.at[n_dp]).wait_send()
    awaited(routes.at[:, near_parts], route_send).wait_send()
    awaited(routes.at[0, pl.ds(0, n_dp - 1)], far_send).wait_send()
    awaited(own, z_send).wait_send()
    awaited(message.at[0, near_parts], part_send.at[0]).wait_send()
    awaited(message.at[far_parts], part_send.at[1]).wait_send()
    awaited(proj.at[far_parts], proj_send).wait_send()
    pltpu.make_async_copy(basis, basis_ref, out_sem.at[0]).wait()
    pltpu.make_async_copy(upd, upd_ref, out_sem.at[1]).wait()


def fused_buffers(n_expert, n_dp, tokens, width, experts, slots, units, rank, top):
    cols = width // n_dp
    halves = ((2 * experts, rank // 2, units), BF16)
    flat = (rank * 3 // 2, 128) if 2 * slots == 3 * 128 and rank % 32 == 0 else (rank, slots)
    return [
        ((n_dp, n_expert, tokens, cols), BF16),
        ((n_dp - 1, tokens, cols), BF16),
        ((experts, slots, units), BF16),
        ((n_expert, experts * rank, cols), BF16),
        ((n_dp, n_expert, 2 * top, tokens), F32),
        ((n_dp, experts, n_expert * tokens), F32),
        ((n_dp, experts, slots, n_expert * tokens), BF16),
        ((n_dp, n_expert * experts, tokens), F32),
        ((n_dp, n_expert, slots, tokens), BF16),
        ((2, n_expert, experts * rank, tokens), BF16),
        ((n_dp, n_expert, *flat), BF16),
        ((n_dp, n_expert, *flat), BF16),
        ((experts, slots, slots), BF16),
        halves,
        halves,
        halves,
        halves,
        ((experts, rank, 2 * rank), F32),
        ((n_dp, experts // 2, rank, 2 * slots), BF16),
        ((experts * rank, n_expert * tokens), BF16),
        ((experts, rank, units), F32),
        ((experts * rank, cols), F32),
    ]


def fused(grads, ids, probs, hidden, q, buffers):
    n_expert, n_dp = lax.axis_size("expert"), lax.axis_size("dp")
    experts, slots, units = hidden.shape
    rank = q.shape[0] // experts
    cols = q.shape[1] // n_dp
    chips = n_expert // 2
    long = max(math.isqrt(chips), chips // math.isqrt(chips))
    tags = n_dp + 1
    dma = pltpu.SemaphoreType.DMA
    vmem = pl.BlockSpec(memory_space=pltpu.VMEM)
    anywhere = pl.BlockSpec(memory_space=pl.ANY)
    return pl.pallas_call(
        functools.partial(fused_kernel, n_expert, n_dp),
        out_shape=(
            jax.ShapeDtypeStruct((experts, rank, units), F32),
            jax.ShapeDtypeStruct((experts * rank, cols), F32),
        ),
        in_specs=[anywhere, vmem, vmem, anywhere, anywhere],
        out_specs=(anywhere, anywhere),
        scratch_shapes=[pltpu.VMEM(*b) for b in buffers] + [
            pltpu.SemaphoreType.REGULAR, dma((2,)), dma((n_dp + 2,)),
            dma(()), dma((n_dp,)), dma(()), dma((n_dp,)), dma(()), dma((n_dp,)),
            dma((tags,)), dma((2, tags, long - 1)), dma((2, tags, long, long - 1)), dma((tags,)),
            dma((2,)), dma((2,)), dma((3,)), dma((3, 2 * experts)), dma(()), dma((n_dp,)),
        ],
        compiler_params=pltpu.CompilerParams(
            collective_id=2, has_side_effects=True, vmem_limit_bytes=67043328
        ),
        name="fused",
    )(grads, ids, probs, hidden, q)


def local(out_grads, expert_ids, gate_probs, hidden_acts, q_previous):
    n_expert, n_dp = lax.axis_size("expert"), lax.axis_size("dp")
    experts, slots, units = hidden_acts.shape[1:]
    tokens, width = out_grads.shape[1:]
    rank = q_previous.shape[1]
    cols = width // n_dp
    buffers = fused_buffers(
        n_expert, n_dp, tokens, width, experts, slots, units, rank, expert_ids.shape[2]
    )
    held = sum(math.prod(shape) * jnp.dtype(kind).itemsize for shape, kind in buffers)
    if n_dp != 4 or held > 60 * 2**20:
        return spacious(out_grads, expert_ids, gate_probs, hidden_acts, q_previous)
    q = q_previous.reshape(experts * rank, width)
    basis, update = fused(out_grads[0], expert_ids[0].T, gate_probs[0].T, hidden_acts[0], q, buffers)
    return (basis, update.reshape(experts, rank, cols))


def spacious(out_grads, expert_ids, gate_probs, hidden_acts, q_previous):
    n_expert = lax.axis_size("expert")
    n_dp = lax.axis_size("dp")
    experts, slots, units = hidden_acts.shape[1:]
    capacity = slots // n_expert
    tokens, width = out_grads.shape[1:]
    top = expert_ids.shape[2]
    rank = q_previous.shape[1]
    cols = width // n_dp
    first = lax.axis_index("expert") * experts

    route = jnp.concatenate([expert_ids[0].astype(F32), gate_probs[0]], axis=1).T
    grads, route = gathered(out_grads[0], route)
    mine = (first + jnp.arange(experts)).astype(F32)[:, None]
    ids = route[:, :, :top].transpose(2, 0, 1, 3)[:, :, :, None, :]
    weight = route[:, :, top:].transpose(2, 0, 1, 3)[:, :, :, None, :]
    hit = ids == mine
    gate = jnp.sum(jnp.where(hit, weight, 0.0), axis=0)
    chosen = jnp.any(hit, axis=0)
    earlier = (jnp.arange(tokens)[:, None] < jnp.arange(tokens)[None, :]).astype(BF16)
    place = jnp.einsum("pbjt,tu->pbju", chosen.astype(BF16), earlier, preferred_element_type=F32)
    place = jnp.where(chosen, place, -1.0)
    pick = (place[:, :, :, None, :] == jnp.arange(capacity, dtype=F32)[:, None]).astype(BF16)

    q_part = lax.dynamic_slice_in_dim(q_previous, lax.axis_index("dp") * cols, cols, 2)
    mixed = jnp.einsum("jrd,bptd->jrbpt", q_part, grads, preferred_element_type=F32)
    scale = gate.transpose(2, 1, 0, 3)
    mixed = (mixed * scale[:, None]).astype(BF16)
    part = jnp.einsum("jrbpt,pbjct->pjrbc", mixed, pick, preferred_element_type=F32).astype(BF16)
    part = part.reshape(n_dp, experts, rank, slots)
    ortho, proj = factors(part, hidden_acts[0], n_dp)
    proj = proj.reshape(n_dp, experts, rank, n_expert, capacity)
    spread = jnp.einsum("pjrbc,pbjct->jrbpt", proj, pick, preferred_element_type=F32)
    spread = (spread * scale[:, None]).astype(BF16)
    q_update = jnp.einsum("jrbpt,bptd->jrd", spread, grads, preferred_element_type=F32)
    new_basis = ortho.astype(F32) * math.sqrt(units)
    return (new_basis, q_update)


def solution(mesh):
    return jax.shard_map(
        local,
        mesh=mesh,
        in_specs=(
            P("dp", "expert", None),
            P("dp", "expert", None),
            P("dp", "expert", None),
            P("dp", "expert", None, None),
            P("expert", None, None),
        ),
        out_specs=(P("expert", None, None), P("expert", None, "dp")),
        check_vma=False,
    )
```
